128 devices in a mesh: front: 8 (over y_hi, z), tile: 16 (over x, y_lo, core).
Axes of the slice: x: 4, y: 4 (y_hi: 2, y_lo: 2; y = y_hi * 2 + y_lo), z: 4, core: 2. Of those that a mesh axis runs over, the one named last changes fastest.
Arguments:
- lower_basis: bfloat16 [8, 16, 512, 1024], P('front', 'tile'), may hold values from -0.75 to 0.75
- lower_coeff: bfloat16 [8, 16, 512, 1024], P('front', 'tile'), may hold values from -0.75 to 0.75
- upper_basis: bfloat16 [8, 16, 512, 1024], P('front', 'tile'), may hold values from -0.75 to 0.75
- upper_coeff: bfloat16 [8, 16, 512, 1024], P('front', 'tile'), may hold values from -0.75 to 0.75
- lower_rank: int32 [8, 16, 32], P('front', 'tile'), may hold values from 1 to 32
- upper_rank: int32 [8, 16, 32], P('front', 'tile'), may hold values from 1 to 32
- child_half: int32 [8, 16], replicated, may hold values from 0 to 1
- owner_shift: int32 [2, 32], replicated, may hold values from 0 to 3
Outputs:
- parent_tiles: bfloat16 [8, 16, 8192, 512], P('front', 'tile')
The draws below stay inside these ranges and needn't reach their ends.
Inputs may be any that keep to these rules, and one draw needn't show every extreme that they name: `child_half`: 0 keeps a tile's index, 1 moves it by 16.
All inputs are finite; a program needn't handle non-finite values.
Results may differ from the reference program's by a relative error of at most 0.0062.
Values may be sent and summed in bfloat16 or wider, within the bound.
A program may use at most 192 MiB of HBM per device.

```python
import jax
import jax.numpy as jnp
from jax import lax

B = 512
R = 32
KP = 32
K = 1024
NC = 16
PT = 32
FRONTS = 8
PARENTS = 2


def touch_ends(entries, own_key, smallest, top_value):
    dims = entries.shape
    index_at = [jax.random.randint(jax.random.fold_in(own_key, axis), (), 0, dims[axis]) for axis in range(len(dims))]
    entries = entries.at[tuple(index_at)].set(smallest)
    longest = dims.index(max(dims))
    index_at[longest] = (index_at[longest] + 1) % dims[longest]
    return entries.at[tuple(index_at)].set(top_value)


def steps_of(key, extent, pieces, low, largest):
    level = 1.0
    for dim, parts in pieces:
        heights = jax.random.uniform(jax.random.fold_in(jax.random.fold_in(key, 6), dim), (parts,), jnp.float32, low / len(pieces), largest / len(pieces))
        level = level * jnp.repeat(jnp.exp(heights), extent[dim] // parts).reshape((-1,) + (1,) * (len(extent) - 1 - dim))
    return level


def bell_draw(stream_key, extent, deviation, limit, cuts=(), kind=jnp.bfloat16):
    drawn = deviation * jax.random.normal(stream_key, extent, jnp.float32)
    if cuts:
        drawn = drawn * steps_of(stream_key, extent, cuts, -0.22, 0.18)
    return jnp.clip(drawn, -limit, limit).astype(kind)


def setup_inputs(seed: int = 0) -> dict:
    keys = jax.random.split(jax.random.key(seed), 9)
    lower_basis = bell_draw(keys[0], (FRONTS, NC, B, K), ((KP * R * R * B) ** -0.125), 0.75, ((0, 8), (1, 16)))
    lower_coeff = bell_draw(keys[1], (FRONTS, NC, B, K), ((KP * R * R * B) ** -0.125), 0.75, ((0, 8), (1, 16)))
    upper_basis = bell_draw(keys[2], (FRONTS, NC, B, K), ((KP * R * R * B) ** -0.125), 0.75, ((0, 8), (1, 16)))
    upper_coeff = bell_draw(keys[3], (FRONTS, NC, B, K), ((KP * R * R * B) ** -0.125), 0.75, ((0, 8), (1, 16)))
    lower_rank = touch_ends(jax.random.randint(keys[4], (FRONTS, NC, KP), 1, R + 1), jax.random.fold_in(keys[4], 1), 1, R).astype(jnp.int32)
    upper_rank = touch_ends(jax.random.randint(keys[5], (FRONTS, NC, KP), 1, R + 1), jax.random.fold_in(keys[5], 1), 1, R).astype(jnp.int32)
    child_half = touch_ends(jax.random.randint(keys[6], (FRONTS, NC), 0, 2), jax.random.fold_in(keys[6], 1), 0, 1).astype(jnp.int32)
    owner_shift = touch_ends(jax.random.randint(keys[7], (PARENTS, PT), 0, 4), jax.random.fold_in(keys[7], 1), 0, 3).astype(jnp.int32)
    return {"lower_basis": lower_basis, "lower_coeff": lower_coeff, "upper_basis": upper_basis, "upper_coeff": upper_coeff, "lower_rank": lower_rank, "upper_rank": upper_rank, "child_half": child_half, "owner_shift": owner_shift}


def masked(basis, ranks):
    keep = (jnp.arange(R, dtype=jnp.int32)[None, None, :] < ranks[:, :, None]).astype(jnp.float32)
    rows = basis.shape[0]
    return basis.astype(jnp.float32).reshape(rows, B, KP, R) * keep[:, None]


def front_tiles(lower_basis, lower_coeff, upper_basis, upper_coeff, lower_rank, upper_rank):
    lower_kept = masked(lower_basis, lower_rank)
    coeff_rows = lower_coeff.astype(jnp.float32).reshape(NC, B, KP, R)

    def column(packed):
        upper_one, coeff_one, col_ranks = packed
        upper_rows = upper_one.astype(jnp.float32).reshape(B, KP, R)
        upper_kept = masked(coeff_one[None], col_ranks[None])[0].reshape(B, KP * R)
        middle = jnp.einsum('ibkr,bks->ikrs', coeff_rows, upper_rows).astype(jnp.bfloat16)
        middle = lax.optimization_barrier(middle).astype(jnp.float32)
        widened = jnp.einsum('ibkr,ikrs->ibks', lower_kept, middle).astype(jnp.bfloat16)
        widened = lax.optimization_barrier(widened).astype(jnp.float32).reshape(NC, B, KP * R)
        return jnp.einsum('ibk,ck->ibc', widened, upper_kept).astype(jnp.bfloat16)

    return lax.map(column, (upper_basis, upper_coeff, upper_rank))


def reference(lower_basis, lower_coeff, upper_basis, upper_coeff, lower_rank, upper_rank, child_half, owner_shift):
    all_tiles = lax.map(lambda packed: front_tiles(*packed),
                        (lower_basis, lower_coeff, upper_basis, upper_coeff, lower_rank, upper_rank))
    half_rows = NC // 2
    col_ids = jnp.arange(NC, dtype=jnp.int32)[:, None]
    slot_ids = jnp.arange(NC, dtype=jnp.int32)[None, :]
    col_half = slot_ids // half_rows
    row_group = slot_ids % half_rows
    parent_col = col_ids + NC * col_half

    def receiver(out_front):
        parent = out_front // 4
        offset = out_front % 4
        shifts = lax.dynamic_index_in_dim(owner_shift, parent, 0, keepdims=False)
        parent_row = 4 * row_group + (offset - shifts[parent_col]) % 4
        child_row = parent_row % NC
        row_half = parent_row // NC
        assembled = jnp.zeros((NC, NC, B, B), jnp.float32)
        for sibling in range(4):
            child_front = 4 * parent + sibling
            tiles = lax.dynamic_index_in_dim(all_tiles, child_front, 0, keepdims=False)
            halves = lax.dynamic_index_in_dim(child_half, child_front, 0, keepdims=False)
            matches = (halves[col_ids] == col_half) & (halves[child_row] == row_half)
            picked = tiles[col_ids, child_row].astype(jnp.float32)
            assembled = assembled + jnp.where(matches[:, :, None, None], picked, jnp.float32(0.0))
        return assembled.astype(jnp.bfloat16).reshape(NC, NC * B, B)

    return lax.map(receiver, jnp.arange(FRONTS, dtype=jnp.int32))
```

```python
import functools

import jax
import jax.numpy as jnp
from jax import lax
from jax.experimental import pallas as pl
from jax.experimental.pallas import tpu as pltpu
from jax.sharding import PartitionSpec as P

MESH = pl.DeviceIdType.MESH
B = 512
R = 32
KP = 32
K = 1024
CH = 4
PR = B // CH
HR = PR // 2
BF = jnp.bfloat16

Y_OPS = (
    [("Y", 0, 0, k) for k in range(CH)]
    + [("X", 0, 0, k) for k in range(CH)]
    + [("X", d, 0, k) for k in range(CH) for d in (1, -1)]
    + [("X", 2, 0, 1), ("X", 2, 0, 3)]
)


def x_ops(sign):
    first = (0, 1) if sign > 0 else (2, 3)
    return (
        [("Y", 0, 0, k) for k in range(CH)]
        + [("Y", 0, 1, k) for k in range(CH)]
        + [("X", 0, 0, k) for k in range(CH)]
        + [("Y", -sign, 0, k) for k in first]
        + [("Y", -sign, 1, k) for k in first]
        + [("X", -sign, 0, k) for k in first[::-1]]
        + [("X", -sign, 1, first[0])]
    )


LINK_OPS = [("y",) + op for op in Y_OPS] + [("+",) + op for op in x_ops(1)] + [("-",) + op for op in x_ops(-1)]
LINK_ID = {op: i for i, op in enumerate(LINK_OPS)}
CORE_OPS = [(kind, dx, dy, k) for kind in "YX" for dx in (0, 1, -1, 2) for dy in (0, 1) for k in range(CH)]
CORE_ID = {op: i for i, op in enumerate(CORE_OPS)}
Z_STEPS = (
    [(0, k) for k in range(CH)]
    + [(d, k) for k in range(CH) for d in (1, -1)]
    + [(2, k) for k in (1, 3, 0, 2)]
)
V_SLOT = {0: 0, 1: 1, -1: 2, 2: 0}


def main_kernel(
    lrank, urank, halves, shifts, xin, yin, pin, qin, out,
    xbuf, ybuf, vbuf, pbuf, ptbuf, qbuf, stage, sbuf, relay,
    in_sem, ls, lr, cs, cr, zs, zr, os_sem,
):
    front, tile = lax.axis_index("front"), lax.axis_index("tile")
    yh, z = front // 4, front % 4
    x, yl, core = tile // 4, (tile // 2) % 2, tile % 2

    def tile_at(gx, gy, gc):
        return (gx * 2 + gy) * 2 + gc

    dev = {
        "y": (front, tile_at(x, 1 - yl, core)),
        "+": (front, tile_at((x + 1) % 4, yl, core)),
        "-": (front, tile_at((x + 3) % 4, yl, core)),
        "c": (front, tile_at(x, yl, 1 - core)),
        "z+": (yh * 4 + (z + 1) % 4, tile),
        "z-": (yh * 4 + (z + 3) % 4, tile),
    }

    def row_of(dx, dy, gc):
        gy = yl if dy == 0 else 1 - yl
        return tile_at((x + dx + 4) % 4, gy, gc)

    bufs = {"X": xbuf, "Y": ybuf}

    def piece(kind, dx, dy, gc, k):
        return bufs[kind].at[row_of(dx, dy, gc), pl.ds(k * PR, PR), :]

    sends = []

    def link_copy(op):
        link, kind, dx, dy, k = op
        ref = piece(kind, dx, dy, core, k)
        i = LINK_ID[op]
        return pltpu.make_async_remote_copy(
            src_ref=ref, dst_ref=ref, send_sem=ls.at[i], recv_sem=lr.at[i],
            device_id=dev[link], device_id_type=MESH,
        )

    def send(link, kind, dx, dy, k):
        copy = link_copy((link, kind, dx, dy, k))
        copy.start()
        sends.append(copy)

    def core_send(kind, dx, dy, k):
        i = CORE_ID[(kind, dx, dy, k)]
        ref = piece(kind, dx, dy, core, k)
        copy = pltpu.make_async_remote_copy(
            src_ref=ref, dst_ref=ref, send_sem=cs.at[i], recv_sem=cr.at[i],
            device_id=dev["c"], device_id_type=MESH,
        )
        copy.start()
        sends.append(copy)

    def core_recv(kind, dx, dy, k):
        i = CORE_ID[(kind, dx, dy, k)]
        ref = piece(kind, dx, dy, 1 - core, k)
        pltpu.make_async_remote_copy(
            src_ref=ref, dst_ref=ref, send_sem=cs.at[i], recv_sem=cr.at[i],
            device_id=dev["c"], device_id_type=MESH,
        ).wait_recv()

    def recv(link, kind, dx, dy, k):
        if link == "y":
            sender = (kind, dx, 1 - dy, k)
        elif link == "+":
            sender = (kind, (dx + 1 + 1) % 4 - 1, dy, k)
        else:
            sender = (kind, (dx - 1 + 1) % 4 - 1, dy, k)
        i = LINK_ID[(link,) + sender]
        ref = piece(kind, dx, dy, core, k)
        pltpu.make_async_remote_copy(
            src_ref=ref, dst_ref=ref, send_sem=ls.at[i], recv_sem=lr.at[i],
            device_id=dev[link], device_id_type=MESH,
        ).wait_recv()
        core_send(kind, dx, dy, k)

    me = tile
    y_loads = []
    for k in range(CH):
        rows = pl.ds(k * PR, PR)
        copy = pltpu.make_async_copy(yin.at[rows, :], ybuf.at[me, rows, :], in_sem.at[k])
        copy.start()
        y_loads.append(copy)
    x_load = pltpu.make_async_copy(xin, xbuf.at[me], in_sem.at[CH])
    p_load = pltpu.make_async_copy(pin, pbuf, in_sem.at[CH + 1])
    q_load = pltpu.make_async_copy(qin, qbuf, in_sem.at[CH + 2])
    x_load.start()
    p_load.start()
    q_load.start()

    barrier = pltpu.get_barrier_semaphore()
    for name in ("y", "+", "-", "c", "z+", "z-"):
        pl.semaphore_signal(barrier, inc=1, device_id=dev[name], device_id_type=MESH)

    col = lax.broadcasted_iota(jnp.int32, (8, K), 1)

    def keep(ranks):
        limit = jnp.zeros((8, K), jnp.int32)
        for k in range(KP):
            limit = jnp.where(col // R == k, ranks[k], limit)
        return (col % R < limit).astype(jnp.float32)

    lkeep = keep(lrank)[:1]
    ukeep = keep(urank)[:1]
    pl.semaphore_wait(barrier, 6)

    def mask_y(k):
        y_loads[k].wait()
        rows = pl.ds(k * PR, PR)
        ybuf[me, rows, :] = (ybuf[me, rows, :].astype(jnp.float32) * lkeep).astype(BF)

    def send_own_y(k):
        for link in ("y", "+", "-"):
            send(link, "Y", 0, 0, k)
        core_send("Y", 0, 0, k)

    mask_y(0)
    for k in range(1, CH):
        mask_y(k)
        send_own_y(k - 1)
    x_load.wait()
    send_own_y(CH - 1)
    for k in range(CH):
        send("y", "X", 0, 0, k)
        core_send("X", 0, 0, k)

    p_load.wait()
    for q in range(4):
        cols = slice(q * 256, (q + 1) * 256)
        part = pbuf[:, cols].astype(jnp.float32) * ukeep[:, cols]
        ptbuf[cols, :] = part.T.astype(BF)
    q_load.wait()

    def same_panel():
        a = lax.broadcasted_iota(jnp.int32, (256, 256), 0) // R
        b = lax.broadcasted_iota(jnp.int32, (256, 256), 1) // R
        return a == b

    def make_v(dx, dy, classes=(0, 1)):
        slot = V_SLOT[dx]
        gy = yl if dy == 0 else 1 - yl

        def body(n, carry):
            gc = (core + classes[0] + n // 4) % 2
            q = n % 4
            cols = pl.ds(pl.multiple_of(q * 256, 256), 256)
            row = tile_at((x + dx + 4) % 4, gy, gc)
            mt = jnp.dot(ptbuf[cols, :], ybuf[row, :, cols], preferred_element_type=jnp.float32)
            mt = jnp.where(same_panel(), mt, 0.0).astype(BF)
            v = jnp.dot(qbuf[:, cols], mt, preferred_element_type=jnp.float32)
            vbuf[slot, gy * 2 + gc, :, cols] = v.astype(BF)
            return carry

        lax.fori_loop(0, 4 * len(classes), body, 0)

    half = halves[front, tile]
    shift = shifts[yh, tile + 16 * half]
    z_copies = []
    own_copies = []

    def z_copy(n, what, src, dst, to):
        return pltpu.make_async_remote_copy(
            src_ref=src, dst_ref=dst, send_sem=zs.at[n, what], recv_sem=zr.at[n, what],
            device_id=dev[to], device_id_type=MESH,
        )

    def z_refs(n, what, receiving=False):
        dx, k = Z_STEPS[n]
        g = (x + dx + 4) % 4
        back = (z + 3) % 4 if receiving else z
        ahead = (z + 1) % 4 if receiving else z
        if what == 0:
            return sbuf.at[n, 2, pl.ds(0, HR), :], relay.at[n, 0], "z+"
        if what == 1:
            return sbuf.at[n, 2, pl.ds(HR, HR), :], relay.at[n, 1], "z-"
        if what == 2:
            return sbuf.at[n, 1], out.at[back, g, pl.ds(k * PR, PR), :], "z+"
        if what == 3:
            return sbuf.at[n, 3], out.at[ahead, g, pl.ds(k * PR, PR), :], "z-"
        if what == 4:
            child = (z + 2) % 4 if receiving else (z + 3) % 4
            return relay.at[n, 0], out.at[child, g, pl.ds(k * PR, HR), :], "z+"
        child = (z + 2) % 4 if receiving else (z + 1) % 4
        return relay.at[n, 1], out.at[child, g, pl.ds(k * PR + HR, HR), :], "z-"

    def z_send(n, what):
        src, dst, to = z_refs(n, what)
        copy = z_copy(n, what, src, dst, to)
        copy.start()
        sends.append(copy)

    def z_wait(n, what):
        src, dst, to = z_refs(n, what, receiving=True)
        z_copy(n, what, src, dst, to).wait_recv()

    def hand_on(n):
        for what in (0, 1):
            z_wait(n, what)
            z_send(n, what + 4)

    def z_step(n):
        dx, k = Z_STEPS[n]
        slot = V_SLOT[dx]
        g = (x + dx + 4) % 4

        def body(r, carry):
            acc = lax.dot_general(
                xbuf[g * 4 + r, pl.ds(k * PR, PR), :],
                vbuf[slot, r],
                (((1,), (1,)), ((), ())),
                preferred_element_type=jnp.float32,
            )
            stage[r] = acc.astype(BF)
            return carry

        lax.fori_loop(0, 4, body, 0)
        for rel in (2, 1, 3, 0):
            sbuf[n, rel] = stage[(z + rel - shift + 4) % 4]
        for what in (0, 1, 2, 3):
            z_send(n, what)
        copy = pltpu.make_async_copy(sbuf.at[n, 0], out.at[z, g, pl.ds(k * PR, PR), :], os_sem.at[n])
        copy.start()
        own_copies.append(copy)
        if n > 0:
            hand_on(n - 1)

    for k in range(CH):
        core_recv("Y", 0, 0, k)
    make_v(0, 0)
    for k in range(CH):
        recv("y", "Y", 0, 1, k)
        send("+", "Y", 0, 1, k)
        send("-", "Y", 0, 1, k)
        recv("+", "Y", -1, 0, k)
        recv("-", "Y", 1, 0, k)
    for k in range(CH):
        send("+", "X", 0, 0, k)
        send("-", "X", 0, 0, k)
    for k in range(CH):
        core_recv("Y", 0, 1, k)
    make_v(0, 1)
    for k in range(CH):
        recv("y", "X", 0, 1, k)
        recv("+", "Y", -1, 1, k)
        recv("-", "Y", 1, 1, k)
        core_recv("X", 0, 0, k)
        core_recv("X", 0, 1, k)
        z_step(k)
        if k in (1, 2):
            d = 1 if k == 1 else -1
            for j in range(CH):
                core_recv("Y", d, 0, j)
            make_v(d, 0)
    for d in (1, -1):
        for k in range(CH):
            core_recv("Y", d, 1, k)
        make_v(d, 1)
    for k in range(CH):
        recv("-", "X", 1, 0, k)
        send("y", "X", 1, 0, k)
        recv("+", "X", -1, 0, k)
        send("y", "X", -1, 0, k)
        if k == 0:
            for j in (0, 1):
                send("+", "Y", -1, 0, j)
                send("-", "Y", 1, 0, j + 2)
            for j in (0, 1):
                send("+", "Y", -1, 1, j)
                send("-", "Y", 1, 1, j + 2)
        if k == 3:
            for j in (1, 0):
                send("+", "X", -1, 0, j)
                send("-", "X", 1, 0, j + 2)
        if k >= 1:
            n = CH + 2 * (k - 1)
            for d in (1, -1):
                recv("y", "X", d, 1, k - 1)
                core_recv("X", d, 0, k - 1)
                core_recv("X", d, 1, k - 1)
                z_step(n + (d < 0))
    send("+", "X", -1, 1, 0)
    send("-", "X", 1, 1, 2)
    for j in (0, 1):
        recv("+", "Y", 2, 0, j)
        recv("-", "Y", 2, 0, j + 2)
    for d in (1, -1):
        recv("y", "X", d, 1, 3)
        core_recv("X", d, 0, 3)
        core_recv("X", d, 1, 3)
        z_step(CH + 6 + (d < 0))
        if d == 1:
            for j in range(CH):
                core_recv("Y", 2, 0, j)
            make_v(2, 0)
    for j in (0, 1):
        recv("+", "Y", 2, 1, j)
        recv("-", "Y", 2, 1, j + 2)
    for j in range(CH):
        core_recv("Y", 2, 1, j)
    make_v(2, 1)
    recv("+", "X", 2, 0, 1)
    send("y", "X", 2, 0, 1)
    recv("-", "X", 2, 0, 3)
    send("y", "X", 2, 0, 3)
    recv("+", "X", 2, 0, 0)
    recv("-", "X", 2, 0, 2)
    recv("y", "X", 2, 1, 1)
    recv("+", "X", 2, 1, 0)
    recv("-", "X", 2, 1, 2)
    recv("y", "X", 2, 1, 3)
    for n in range(3 * CH, 4 * CH):
        core_recv("X", 2, 0, Z_STEPS[n][1])
        core_recv("X", 2, 1, Z_STEPS[n][1])
        z_step(n)
    hand_on(4 * CH - 1)
    for n in range(4 * CH):
        for what in (2, 3, 4, 5):
            z_wait(n, what)
    for copy in own_copies:
        copy.wait()
    for copy in sends:
        copy.wait_send()


def main_call(xin, yin, pin, qin, lrank, urank, halves, shifts):
    hbm = pl.BlockSpec(memory_space=pl.ANY)
    smem = pl.BlockSpec(memory_space=pltpu.SMEM)
    steps = 4 * CH
    return pl.pallas_call(
        main_kernel,
        out_shape=jax.ShapeDtypeStruct((4, 4, B, B), BF),
        in_specs=[smem] * 4 + [hbm] * 4,
        out_specs=hbm,
        scratch_shapes=[
            pltpu.VMEM((16, B, K), BF),
            pltpu.VMEM((16, B, K), BF),
            pltpu.VMEM((3, 4, B, K), BF),
            pltpu.VMEM((B, K), BF),
            pltpu.VMEM((K, B), BF),
            pltpu.VMEM((B, K), BF),
            pltpu.VMEM((4, PR, B), BF),
            pltpu.VMEM((steps, 4, PR, B), BF),
            pltpu.VMEM((steps, 2, HR, B), BF),
            pltpu.SemaphoreType.DMA((CH + 3,)),
            pltpu.SemaphoreType.DMA((len(LINK_OPS),)),
            pltpu.SemaphoreType.DMA((len(LINK_OPS),)),
            pltpu.SemaphoreType.DMA((len(CORE_OPS),)),
            pltpu.SemaphoreType.DMA((len(CORE_OPS),)),
            pltpu.SemaphoreType.DMA((steps, 6)),
            pltpu.SemaphoreType.DMA((steps, 6)),
            pltpu.SemaphoreType.DMA((steps,)),
        ],
        compiler_params=pltpu.CompilerParams(
            collective_id=0, has_side_effects=True, vmem_limit_bytes=64_000_000
        ),
        name="gather_update_exchange",
    )(lrank, urank, halves, shifts, xin, yin, pin, qin)


def sum_kernel(halves, shifts, blocks, out):
    front, tile = lax.axis_index("front"), lax.axis_index("tile")
    parent, o = front // 4, front % 4
    g = pl.program_id(0)
    place = []
    for c in range(4):
        child = 4 * parent + c
        col_half = halves[child, tile]
        row = 4 * g + (o - shifts[parent, tile + 16 * col_half] + 4) % 4
        place.append(2 * col_half + halves[child, row])
    for s in range(4):
        total = jnp.zeros(blocks.shape[2:], jnp.float32)
        for c in range(4):
            total = total + jnp.where(place[c] == s, blocks[c, 0].astype(jnp.float32), 0.0)
        out[s, 0] = total.astype(BF)


def sum_call(halves, shifts, blocks):
    rows = B // 2
    smem = pl.BlockSpec(memory_space=pltpu.SMEM)
    block = pl.BlockSpec((4, 1, rows, B), lambda g, i: (0, g, i, 0))
    return pl.pallas_call(
        sum_kernel,
        grid=(4, 2),
        out_shape=jax.ShapeDtypeStruct((4, 4, B, B), BF),
        in_specs=[smem, smem, block],
        out_specs=block,
        name="sum_into_slots",
    )(halves, shifts, blocks)


def per_device(lower_basis, lower_coeff, upper_basis, upper_coeff, lower_rank, upper_rank, child_half, owner_shift):
    blocks = main_call(
        lower_basis[0, 0], lower_coeff[0, 0], upper_basis[0, 0], upper_coeff[0, 0],
        lower_rank[0, 0], upper_rank[0, 0], child_half, owner_shift,
    )
    return sum_call(child_half, owner_shift, blocks).reshape(1, 1, 16 * B, B)


def solution(mesh):
    whole = P("front", "tile", None, None)
    ranks = P("front", "tile", None)
    return jax.shard_map(
        per_device,
        mesh=mesh,
        in_specs=(whole, whole, whole, whole, ranks, ranks, P(), P()),
        out_specs=whole,
        check_vma=False,
    )
```

```python
import functools

import jax
import jax.numpy as jnp
from jax import lax
from jax.experimental import pallas as pl
from jax.experimental.pallas import tpu as pltpu
from jax.sharding import PartitionSpec as P

MESH = pl.DeviceIdType.MESH
B = 512
R = 32
KP = 32
K = 1024
CH = 4
PR = B // CH
HR = PR // 2
PK = K // CH
BF = jnp.bfloat16

Y_OPS = (
    [("Y", 0, 0, k) for k in range(CH)]
    + [("X", 0, 0, k) for k in range(CH)]
    + [("X", d, 0, k) for k in range(CH) for d in (1, -1)]
    + [("X", 2, 0, 1), ("X", 2, 0, 3)]
)


def x_ops(sign):
    a, b = (0, 1) if sign > 0 else (2, 3)
    return (
        [("Y", 0, 0, k) for k in range(CH)]
        + [("Y", 0, 1, 0), ("Y", 0, 1, 1)]
        + ([("Y", 0, 1, 2), ("X", 0, 0, 0)] if sign > 0 else [("X", 0, 0, 0), ("Y", 0, 1, 2)])
        + [("Y", 0, 1, 3)]
        + [("X", 0, 0, k) for k in range(1, CH)]
        + [("Y", -sign, 0, a), ("Y", -sign, 0, b), ("Y", -sign, 1, a)]
        + [("X", -sign, 0, b), ("Y", -sign, 1, b), ("X", -sign, 0, a), ("X", -sign, 1, a)]
    )


LINK_OPS = [("y",) + op for op in Y_OPS] + [("+",) + op for op in x_ops(1)] + [("-",) + op for op in x_ops(-1)]
LINK_ID = {op: i for i, op in enumerate(LINK_OPS)}
CORE_OPS = [(kind, dx, dy, k) for kind in "YX" for dx in (0, 1, -1, 2) for dy in (0, 1) for k in range(CH)]
CORE_ID = {op: i for i, op in enumerate(CORE_OPS)}
Z_STEPS = (
    [(0, k) for k in range(CH)]
    + [(d, k) for k in range(CH) for d in (1, -1)]
    + [(2, k) for k in (1, 3, 0, 2)]
)
V_SLOT = {0: 0, 1: 1, -1: 2, 2: 0}


def main_kernel(
    lrank, urank, halves, shifts, xin, yin, pin, qin, out,
    xbuf, ybuf, vbuf, pbuf, qtbuf, raw, stage, sbuf, relay,
    in_sem, ls, lr, cs, cr, zs, zr, zlast, os_sem,
):
    front, tile = lax.axis_index("front"), lax.axis_index("tile")
    yh, z = front // 4, front % 4
    x, yl, core = tile // 4, (tile // 2) % 2, tile % 2

    def tile_at(gx, gy, gc):
        return (gx * 2 + gy) * 2 + gc

    dev = {
        "y": (front, tile_at(x, 1 - yl, core)),
        "+": (front, tile_at((x + 1) % 4, yl, core)),
        "-": (front, tile_at((x + 3) % 4, yl, core)),
        "c": (front, tile_at(x, yl, 1 - core)),
        "z+": (yh * 4 + (z + 1) % 4, tile),
        "z-": (yh * 4 + (z + 3) % 4, tile),
    }

    def row_of(dx, dy, gc):
        gy = yl if dy == 0 else 1 - yl
        return tile_at((x + dx + 4) % 4, gy, gc)

    def piece(kind, dx, dy, gc, k):
        if kind == "X":
            return xbuf.at[row_of(dx, dy, gc), pl.ds(k * PR, PR), :]
        return ybuf.at[row_of(dx, dy, gc), pl.ds(k * PK, PK), :]

    def copy_of(ref, ssem, rsem, to):
        return pltpu.make_async_remote_copy(
            src_ref=ref, dst_ref=ref, send_sem=ssem, recv_sem=rsem,
            device_id=dev[to], device_id_type=MESH,
        )

    def send(link, kind, dx, dy, k):
        i = LINK_ID[(link, kind, dx, dy, k)]
        copy_of(piece(kind, dx, dy, core, k), ls, lr.at[i], link).start()

    def core_send(kind, dx, dy, k):
        i = CORE_ID[(kind, dx, dy, k)]
        copy_of(piece(kind, dx, dy, core, k), cs, cr.at[i], "c").start()

    def core_recv(kind, dx, dy, k):
        i = CORE_ID[(kind, dx, dy, k)]
        copy = copy_of(piece(kind, dx, dy, 1 - core, k), cs, cr.at[i], "c")
        copy.wait_recv()

    def recv(link, kind, dx, dy, k):
        if link == "y":
            sender = (kind, dx, 1 - dy, k)
        elif link == "+":
            sender = (kind, (dx + 2) % 4 - 1, dy, k)
        else:
            sender = (kind, dx % 4 - 1, dy, k)
        i = LINK_ID[(link,) + sender]
        copy = copy_of(piece(kind, dx, dy, core, k), ls, lr.at[i], link)
        copy.wait_recv()
        core_send(kind, dx, dy, k)

    me = tile
    y_loads = []
    for k in range(CH):
        cols = pl.ds(k * PK, PK)
        copy = pltpu.make_async_copy(yin.at[:, cols], raw.at[0, :, cols], in_sem.at[k])
        copy.start()
        y_loads.append(copy)
    x_load = pltpu.make_async_copy(xin, xbuf.at[me], in_sem.at[CH])
    p_load = pltpu.make_async_copy(pin, pbuf, in_sem.at[CH + 1])
    q_load = pltpu.make_async_copy(qin, raw.at[1], in_sem.at[CH + 2])
    x_load.start()
    p_load.start()
    q_load.start()

    barrier = pltpu.get_barrier_semaphore()
    for name in ("y", "+", "-", "c", "z+", "z-"):
        pl.semaphore_signal(barrier, inc=1, device_id=dev[name], device_id_type=MESH)

    col = lax.broadcasted_iota(jnp.int32, (8, K), 1)

    def keep(ranks):
        limit = jnp.zeros((8, K), jnp.int32)
        for k in range(KP):
            limit = jnp.where(col // R == k, ranks[k], limit)
        return (col % R < limit).astype(jnp.float32)[:1]

    lkeep = keep(lrank)

    def turn_y(k):
        y_loads[k].wait()
        part = raw[0, :, k * PK : (k + 1) * PK].astype(jnp.float32) * lkeep[:, k * PK : (k + 1) * PK]
        ybuf[me, k * PK : (k + 1) * PK, :] = part.T.astype(BF)

    def send_own_y(k):
        for link in ("y", "+", "-"):
            send(link, "Y", 0, 0, k)
        core_send("Y", 0, 0, k)

    turn_y(0)
    pl.semaphore_wait(barrier, 6)
    for k in range(1, CH):
        turn_y(k)
        send_own_y(k - 1)
    x_load.wait()
    send_own_y(CH - 1)
    for k in range(CH):
        send("y", "X", 0, 0, k)
        core_send("X", 0, 0, k)

    ukeep = keep(urank)
    p_load.wait()
    pbuf[...] = (pbuf[...].astype(jnp.float32) * ukeep).astype(BF)
    q_load.wait()
    for k in range(CH):
        cols = slice(k * PK, (k + 1) * PK)
        qtbuf[cols, :] = raw[1, :, cols].astype(jnp.float32).T.astype(BF)

    def make_v(dx, dy, k, classes=(0, 1)):
        slot = V_SLOT[dx]
        gy = yl if dy == 0 else 1 - yl
        rows = slice(k * PK, (k + 1) * PK)
        same = (
            lax.broadcasted_iota(jnp.int32, (PK, PK), 0) // R
            == lax.broadcasted_iota(jnp.int32, (PK, PK), 1) // R
        )
        cores = [core if c == 0 else 1 - core for c in classes]
        middles = []
        for gc in cores:
            m = jnp.dot(
                ybuf[row_of(dx, dy, gc), rows, :], pbuf[:, rows], preferred_element_type=jnp.float32
            )
            middles.append(jnp.where(same, m, 0.0).astype(BF))
        for gc, m in zip(cores, middles):
            v = jnp.dot(m, qtbuf[rows, :], preferred_element_type=jnp.float32)
            vbuf[slot, gy * 2 + gc, rows, :] = v.astype(BF)

    half = halves[front, tile]
    shift = shifts[yh, tile + 16 * half]

    def z_copy(n, what, src, dst, to):
        return pltpu.make_async_remote_copy(
            src_ref=src, dst_ref=dst, send_sem=zs, recv_sem=zr.at[n, what] if what < 2 else zlast,
            device_id=dev[to], device_id_type=MESH,
        )

    def z_refs(n, what, receiving=False):
        dx, k = Z_STEPS[n]
        g = (x + dx + 4) % 4
        back = (z + 3) % 4 if receiving else z
        ahead = (z + 1) % 4 if receiving else z
        if what == 0:
            return sbuf.at[n, 2, pl.ds(0, HR), :], relay.at[n, 0], "z+"
        if what == 1:
            return sbuf.at[n, 2, pl.ds(HR, HR), :], relay.at[n, 1], "z-"
        if what == 2:
            return sbuf.at[n, 1], out.at[back, g, pl.ds(k * PR, PR), :], "z+"
        if what == 3:
            return sbuf.at[n, 3], out.at[ahead, g, pl.ds(k * PR, PR), :], "z-"
        if what == 4:
            child = (z + 2) % 4 if receiving else (z + 3) % 4
            return relay.at[n, 0], out.at[child, g, pl.ds(k * PR, HR), :], "z+"
        child = (z + 2) % 4 if receiving else (z + 1) % 4
        return relay.at[n, 1], out.at[child, g, pl.ds(k * PR + HR, HR), :], "z-"

    def z_send(n, what):
        src, dst, to = z_refs(n, what)
        z_copy(n, what, src, dst, to).start()

    def z_wait(n, what):
        src, dst, to = z_refs(n, what, receiving=True)
        copy = z_copy(n, what, src, dst, to)
        copy.wait_recv()

    def hand_on(n):
        for what in (0, 1):
            z_wait(n, what)
            z_send(n, what + 4)

    def z_step(n):
        dx, k = Z_STEPS[n]
        slot = V_SLOT[dx]
        g = (x + dx + 4) % 4
        core_recv("X", dx, 0, k)
        core_recv("X", dx, 1, k)

        def body(r, carry):
            acc = jnp.dot(
                xbuf[g * 4 + r, pl.ds(k * PR, PR), :], vbuf[slot, r], preferred_element_type=jnp.float32
            )
            stage[r] = acc.astype(BF)
            return carry

        lax.fori_loop(0, 4, body, 0, unroll=2)
        for rel in (2, 1, 3, 0):
            sbuf[n, rel] = stage[(z + rel - shift + 4) % 4]
        for what in (0, 1, 2, 3):
            z_send(n, what)
        pltpu.make_async_copy(sbuf.at[n, 0], out.at[z, g, pl.ds(k * PR, PR), :], os_sem).start()

    def relay_of(n):
        if n >= 0:
            hand_on(n)

    for k in range(CH):
        core_recv("Y", 0, 0, k)
        make_v(0, 0, k)
    for k in range(CH):
        recv("y", "Y", 0, 1, k)
        send("+", "Y", 0, 1, k)
        send("-", "Y", 0, 1, k)
        if k == 1:
            send("-", "X", 0, 0, 0)
        if k == 2:
            send("+", "X", 0, 0, 0)
        if k == 3:
            for j in range(1, CH):
                send("+", "X", 0, 0, j)
                send("-", "X", 0, 0, j)
        recv("+", "Y", -1, 0, k)
        recv("-", "Y", 1, 0, k)
        core_recv("Y", 0, 1, k)
        make_v(0, 1, k)
        if k < 3:
            for d in (1, -1):
                core_recv("Y", d, 0, k)
                make_v(d, 0, k)
    for k in range(CH):
        recv("y", "X", 0, 1, k)
        if k == 2:
            recv("-", "X", 1, 0, 0)
            send("y", "X", 1, 0, 0)
        else:
            recv("-", "Y", 1, 1, min(k, 2))
        if k == 3:
            recv("+", "X", -1, 0, 0)
            send("y", "X", -1, 0, 0)
        else:
            recv("+", "Y", -1, 1, k)
        z_step(k)
        relay_of(k - 1)
        if k == 0:
            for d in (1, -1):
                core_recv("Y", d, 0, 3)
                make_v(d, 0, 3)
        if k < 3:
            core_recv("Y", -1, 1, k)
            make_v(-1, 1, k)
        if k != 2:
            core_recv("Y", 1, 1, min(k, 2))
            make_v(1, 1, min(k, 2))
    for u in range(8, 19):
        if u == 8:
            recv("-", "Y", 1, 1, 3)
            recv("+", "Y", -1, 1, 3)
            core_recv("Y", 1, 1, 3)
            make_v(1, 1, 3)
            for d, sign, a, b in ((-1, "+", 0, 1), (1, "-", 2, 3)):
                send(sign, "Y", d, 0, a)
                send(sign, "Y", d, 0, b)
                send(sign, "Y", d, 1, a)
        elif u <= 11:
            k = u - 8
            recv("-", "X", 1, 0, k)
            send("y", "X", 1, 0, k)
            recv("+", "X", -1, 0, k)
            send("y", "X", -1, 0, k)
            if k == 1:
                send("+", "X", -1, 0, 1)
                send("+", "Y", -1, 1, 1)
                send("+", "X", -1, 0, 0)
            if k == 3:
                send("-", "X", 1, 0, 3)
                send("-", "Y", 1, 1, 3)
                send("-", "X", 1, 0, 2)
        elif u <= 13:
            recv("+", "Y", 2, 0, u - 12)
            recv("-", "Y", 2, 0, u - 10)
        elif u == 14:
            recv("+", "Y", 2, 1, 0)
            recv("-", "Y", 2, 1, 2)
        elif u == 15:
            recv("+", "X", 2, 0, 1)
            send("y", "X", 2, 0, 1)
            recv("-", "X", 2, 0, 3)
            send("y", "X", 2, 0, 3)
        elif u == 16:
            recv("+", "Y", 2, 1, 1)
            recv("-", "Y", 2, 1, 3)
        elif u == 17:
            recv("+", "X", 2, 0, 0)
            recv("-", "X", 2, 0, 2)
        else:
            recv("+", "X", 2, 1, 0)
            recv("-", "X", 2, 1, 2)
        if u < 16:
            d, k = Z_STEPS[u - 4]
            recv("y", "X", d, 1, k)
            if (d, k) == (-1, 0):
                send("+", "X", -1, 1, 0)
            if (d, k) == (1, 2):
                send("-", "X", 1, 1, 2)
        elif u < 18:
            recv("y", "X", 2, 1, 1 if u == 16 else 3)
        if u == 16:
            for k in (1, 3):
                core_recv("Y", 2, 1, k)
                make_v(2, 1, k)
        z_step(u - 4)
        if u < 18:
            relay_of(u - 5)
        if u == 8:
            core_recv("Y", -1, 1, 3)
            make_v(-1, 1, 3)
        if u in (13, 14):
            for k in (0, 2) if u == 13 else (1, 3):
                core_recv("Y", 2, 0, k)
                make_v(2, 0, k)
        if u == 15:
            for k in (0, 2):
                core_recv("Y", 2, 1, k)
                make_v(2, 1, k)
    z_step(4 * CH - 1)
    for n in (13, 14, 15):
        hand_on(n)
    theirs = out.at[pl.ds(0, 3)]
    z_all = pltpu.make_async_remote_copy(
        src_ref=sbuf, dst_ref=theirs, send_sem=zs, recv_sem=zlast, device_id=dev["z+"], device_id_type=MESH
    )
    z_all.wait_recv()
    pltpu.make_async_copy(out.at[0], out.at[0], os_sem).wait()
    copy_of(xbuf.at[pl.ds(0, len(LINK_OPS) // CH)], ls, lr.at[0], "y").wait_send()
    copy_of(xbuf, cs, cr.at[0], "c").wait_send()
    copy_of(sbuf, zs, zlast, "z+").wait_send()


def main_call(xin, yin, pin, qin, lrank, urank, halves, shifts):
    hbm = pl.BlockSpec(memory_space=pl.ANY)
    smem = pl.BlockSpec(memory_space=pltpu.SMEM)
    steps = 4 * CH
    return pl.pallas_call(
        main_kernel,
        out_shape=jax.ShapeDtypeStruct((4, 4, B, B), BF),
        in_specs=[smem] * 4 + [hbm] * 4,
        out_specs=hbm,
        scratch_shapes=[
            pltpu.VMEM((16, B, K), BF),
            pltpu.VMEM((16, K, B), BF),
            pltpu.VMEM((3, 4, K, B), BF),
            pltpu.VMEM((B, K), BF),
            pltpu.VMEM((K, B), BF),
            pltpu.VMEM((2, B, K), BF),
            pltpu.VMEM((4, PR, B), BF),
            pltpu.VMEM((steps, 4, PR, B), BF),
            pltpu.VMEM((steps, 2, HR, B), BF),
            pltpu.SemaphoreType.DMA((CH + 3,)),
            pltpu.SemaphoreType.DMA,
            pltpu.SemaphoreType.DMA((len(LINK_OPS),)),
            pltpu.SemaphoreType.DMA,
            pltpu.SemaphoreType.DMA((len(CORE_OPS),)),
            pltpu.SemaphoreType.DMA,
            pltpu.SemaphoreType.DMA((steps, 2)),
            pltpu.SemaphoreType.DMA,
            pltpu.SemaphoreType.DMA,
        ],
        compiler_params=pltpu.CompilerParams(
            collective_id=0, has_side_effects=True, vmem_limit_bytes=64_000_000
        ),
        name="gather_update_exchange",
    )(lrank, urank, halves, shifts, xin, yin, pin, qin)


def sum_kernel(halves, shifts, blocks, out):
    front, tile = lax.axis_index("front"), lax.axis_index("tile")
    parent, o = front // 4, front % 4
    g = pl.program_id(0)
    place = []
    for c in range(4):
        child = 4 * parent + c
        col_half = halves[child, tile]
        row = 4 * g + (o - shifts[parent, tile + 16 * col_half] + 4) % 4
        place.append(2 * col_half + halves[child, row])
    for s in range(4):
        count = sum((place[c] == s).astype(jnp.int32) for c in range(4))
        only = sum(jnp.where(place[c] == s, c, 0) for c in range(4))

        @pl.when(count == 0)
        def _():
            out[s, 0] = jnp.zeros(out.shape[2:], BF)

        @pl.when(count == 1)
        def _():
            out[s, 0] = blocks[only, 0]

        @pl.when(count > 1)
        def _():
            total = jnp.zeros(blocks.shape[2:], jnp.float32)
            for c in range(4):
                total = total + jnp.where(place[c] == s, blocks[c, 0].astype(jnp.float32), 0.0)
            out[s, 0] = total.astype(BF)


def sum_call(halves, shifts, blocks):
    rows = B // 2
    smem = pl.BlockSpec(memory_space=pltpu.SMEM)
    block = pl.BlockSpec((4, 1, rows, B), lambda g, i: (0, g, i, 0))
    return pl.pallas_call(
        sum_kernel,
        grid=(4, 2),
        out_shape=jax.ShapeDtypeStruct((4, 4, B, B), BF),
        in_specs=[smem, smem, block],
        out_specs=block,
        name="sum_into_slots",
    )(halves, shifts, blocks)


def per_device(lower_basis, lower_coeff, upper_basis, upper_coeff, lower_rank, upper_rank, child_half, owner_shift):
    blocks = main_call(
        lower_basis[0, 0], lower_coeff[0, 0], upper_basis[0, 0], upper_coeff[0, 0],
        lower_rank[0, 0], upper_rank[0, 0], child_half, owner_shift,
    )
    return sum_call(child_half, owner_shift, blocks).reshape(1, 1, 16 * B, B)


def solution(mesh):
    whole = P("front", "tile", None, None)
    ranks = P("front", "tile", None)
    return jax.shard_map(
        per_device,
        mesh=mesh,
        in_specs=(whole, whole, whole, whole, ranks, ranks, P(), P()),
        out_specs=whole,
        check_vma=False,
    )
```

```python
import functools

import jax
import jax.numpy as jnp
from jax import lax
from jax.experimental import pallas as pl
from jax.experimental.pallas import tpu as pltpu
from jax.sharding import PartitionSpec as P

MESH = pl.DeviceIdType.MESH
B = 512
R = 32
KP = 32
K = 1024
CH = 4
PR = B // CH
HR = PR // 2
PK = K // CH
BF = jnp.bfloat16

Y_OPS = (
    [("Y", 0, 0, k) for k in range(CH)]
    + [("X", 0, 0, k) for k in range(CH)]
    + [("X", d, 0, k) for k in range(CH) for d in (1, -1)]
    + [("X", 2, 0, 1), ("X", 2, 0, 3)]
)


def x_ops(sign):
    a, b = (0, 1) if sign > 0 else (2, 3)
    return (
        [("Y", 0, 0, k) for k in range(CH)]
        + [("Y", 0, 1, 0), ("Y", 0, 1, 1)]
        + (
            [("Y", 0, 1, 2), ("X", 0, 0, 0), ("X", 0, 0, 1), ("Y", 0, 1, 3)]
            if sign > 0
            else [("X", 0, 0, 0), ("Y", 0, 1, 2), ("Y", 0, 1, 3), ("X", 0, 0, 1)]
        )
        + [("X", 0, 0, 2), ("X", 0, 0, 3)]
        + [("Y", -sign, 0, a), ("Y", -sign, 0, b), ("X", -sign, 0, b)]
        + [("Y", -sign, 1, a), ("Y", -sign, 1, b), ("X", -sign, 0, a), ("X", -sign, 1, a)]
    )


LINK_OPS = [("y",) + op for op in Y_OPS] + [("+",) + op for op in x_ops(1)] + [("-",) + op for op in x_ops(-1)]
LINK_ID = {op: i for i, op in enumerate(LINK_OPS)}
CORE_OPS = [(kind, dx, dy, k) for kind in "YX" for dx in (0, 1, -1, 2) for dy in (0, 1) for k in range(CH)]
CORE_ID = {op: i for i, op in enumerate(CORE_OPS)}
Z_STEPS = (
    [(0, k) for k in range(CH)]
    + [(1, 0), (-1, 0), (-1, 1), (1, 1), (1, 2), (-1, 2), (1, 3), (-1, 3)]
    + [(2, k) for k in (1, 3, 0, 2)]
)
V_SLOT = {0: 0, 1: 1, -1: 2, 2: 0}


def main_kernel(
    lrank, urank, halves, shifts, xin, yin, pin, qin, out,
    xbuf, ybuf, vbuf, pbuf, qtbuf, stage, sbuf, relay,
    in_sem, ls, lr, cs, cr, zs, zr, zlast,
):
    front, tile = lax.axis_index("front"), lax.axis_index("tile")
    yh, z = front // 4, front % 4
    x, yl, core = tile // 4, (tile // 2) % 2, tile % 2

    def tile_at(gx, gy, gc):
        return (gx * 2 + gy) * 2 + gc

    dev = {
        "y": (front, tile_at(x, 1 - yl, core)),
        "+": (front, tile_at((x + 1) % 4, yl, core)),
        "-": (front, tile_at((x + 3) % 4, yl, core)),
        "c": (front, tile_at(x, yl, 1 - core)),
        "z+": (yh * 4 + (z + 1) % 4, tile),
        "z-": (yh * 4 + (z + 3) % 4, tile),
    }

    def row_of(dx, dy, gc):
        gy = yl if dy == 0 else 1 - yl
        return tile_at((x + dx + 4) % 4, gy, gc)

    def piece(kind, dx, dy, gc, k):
        if kind == "X":
            return xbuf.at[row_of(dx, dy, gc), pl.ds(k * PR, PR), :]
        return ybuf.at[row_of(dx, dy, gc), pl.ds(k * PK, PK), :]

    def copy_of(ref, ssem, rsem, to):
        return pltpu.make_async_remote_copy(
            src_ref=ref, dst_ref=ref, send_sem=ssem, recv_sem=rsem,
            device_id=dev[to], device_id_type=MESH,
        )

    def send(link, kind, dx, dy, k):
        i = LINK_ID[(link, kind, dx, dy, k)]
        copy_of(piece(kind, dx, dy, core, k), ls, lr.at[i], link).start()

    def core_send(kind, dx, dy, k):
        i = CORE_ID[(kind, dx, dy, k)]
        copy_of(piece(kind, dx, dy, core, k), cs, cr.at[i], "c").start()

    def core_recv(kind, dx, dy, k):
        i = CORE_ID[(kind, dx, dy, k)]
        copy = copy_of(piece(kind, dx, dy, 1 - core, k), cs, cr.at[i], "c")
        copy.wait_recv()

    def recv(link, kind, dx, dy, k):
        if link == "y":
            sender = (kind, dx, 1 - dy, k)
        elif link == "+":
            sender = (kind, (dx + 2) % 4 - 1, dy, k)
        else:
            sender = (kind, dx % 4 - 1, dy, k)
        i = LINK_ID[(link,) + sender]
        copy = copy_of(piece(kind, dx, dy, core, k), ls, lr.at[i], link)
        copy.wait_recv()
        core_send(kind, dx, dy, k)

    me = tile

    def raw(n, k):
        return vbuf.at[2, n, pl.ds(k // 2 * B, B), pl.ds(k % 2 * PK, PK)]

    y_loads = []
    for k in range(CH):
        cols = pl.ds(k * PK, PK)
        copy = pltpu.make_async_copy(yin.at[:, cols], raw(0, k), in_sem.at[k])
        copy.start()
        y_loads.append(copy)
    x_load = pltpu.make_async_copy(xin, xbuf.at[me], in_sem.at[CH])
    p_load = pltpu.make_async_copy(pin, pbuf, in_sem.at[CH + 1])
    q_loads = [
        pltpu.make_async_copy(qin.at[:, pl.ds(k * PK, PK)], raw(1, k), in_sem.at[CH + 2 + k])
        for k in range(CH)
    ]
    for copy in [x_load, p_load] + q_loads:
        copy.start()

    barrier = pltpu.get_barrier_semaphore()
    for name in ("y", "+", "-", "c", "z+", "z-"):
        pl.semaphore_signal(barrier, inc=1, device_id=dev[name], device_id_type=MESH)

    col = lax.broadcasted_iota(jnp.int32, (8, K), 1)

    def keep(ranks):
        limit = jnp.zeros((8, K), jnp.int32)
        for k in range(KP):
            limit = jnp.where(col // R == k, ranks[k], limit)
        return (col % R < limit).astype(jnp.float32)[:1]

    lkeep = keep(lrank)

    def turn_y(k):
        y_loads[k].wait()
        part = raw(0, k)[...].astype(jnp.float32) * lkeep[:, k * PK : (k + 1) * PK]
        ybuf[me, k * PK : (k + 1) * PK, :] = part.T.astype(BF)

    def send_own_y(k):
        for link in ("y", "+", "-"):
            send(link, "Y", 0, 0, k)
        core_send("Y", 0, 0, k)

    turn_y(0)
    pl.semaphore_wait(barrier, 6)
    for k in range(1, CH):
        turn_y(k)
        send_own_y(k - 1)
    x_load.wait()
    send_own_y(CH - 1)
    for k in range(CH):
        send("y", "X", 0, 0, k)
        core_send("X", 0, 0, k)

    ukeep = keep(urank)
    p_load.wait()
    pbuf[...] = (pbuf[...].astype(jnp.float32) * ukeep).astype(BF)
    for k in range(CH):
        q_loads[k].wait()
        qtbuf[k * PK : (k + 1) * PK, :] = raw(1, k)[...].astype(jnp.float32).T.astype(BF)

    def make_v(dx, dy, k, classes=(0, 1)):
        slot = V_SLOT[dx]
        gy = yl if dy == 0 else 1 - yl
        rows = slice(k * PK, (k + 1) * PK)
        same = (
            lax.broadcasted_iota(jnp.int32, (PK, PK), 0) // R
            == lax.broadcasted_iota(jnp.int32, (PK, PK), 1) // R
        )
        cores = [core if c == 0 else 1 - core for c in classes]
        middles = []
        for gc in cores:
            m = jnp.dot(
                ybuf[row_of(dx, dy, gc), rows, :], pbuf[:, rows], preferred_element_type=jnp.float32
            )
            middles.append(jnp.where(same, m, 0.0).astype(BF))
        for gc, m in zip(cores, middles):
            v = jnp.dot(m, qtbuf[rows, :], preferred_element_type=jnp.float32)
            vbuf[slot, gy * 2 + gc, rows, :] = v.astype(BF)

    col_half = [halves[4 * yh + c, tile] for c in range(4)]
    col_shift = [shifts[yh, tile + 16 * col_half[c]] for c in range(4)]
    half = halves[front, tile]
    shift = shifts[yh, tile + 16 * half]

    def z_copy(n, what, src, dst, to):
        return pltpu.make_async_remote_copy(
            src_ref=src, dst_ref=dst, send_sem=zs, recv_sem=zr.at[n, what] if what < 2 else zlast.at[n],
            device_id=dev[to], device_id_type=MESH,
        )

    def z_refs(n, what):
        dx, k = Z_STEPS[n]
        g = (x + dx + 4) % 4
        if what == 0:
            return sbuf.at[n, 1, pl.ds(0, HR), :], relay.at[n, 0], "z+"
        if what == 1:
            return sbuf.at[n, 1, pl.ds(HR, HR), :], relay.at[n, 1], "z-"
        if what == 2:
            return sbuf.at[n, 0], out.at[z, g, pl.ds(k * PR, PR), :], "z+"
        if what == 3:
            return sbuf.at[n, 2], out.at[z, g, pl.ds(k * PR, PR), :], "z-"
        if what == 4:
            return relay.at[n, 0], out.at[(z + 3) % 4, g, pl.ds(k * PR, HR), :], "z+"
        return relay.at[n, 1], out.at[(z + 1) % 4, g, pl.ds(k * PR + HR, HR), :], "z-"

    def z_send(n, what):
        src, dst, to = z_refs(n, what)
        z_copy(n, what, src, dst, to).start()

    def z_wait(n, what):
        src, dst, to = z_refs(n, what)
        copy = z_copy(n, what, src, dst, to)
        copy.wait_recv()

    def sum_step(n):
        dx, k = Z_STEPS[n]
        g = (x + dx + 4) % 4
        copy = z_copy(n, 2, sbuf.at[n], out.at[pl.ds(0, 3), g, pl.ds(k * PR, PR), :], "z+")
        copy.wait_recv()
        place = []
        for c in range(4):
            row = 4 * g + (z - col_shift[c] + 4) % 4
            place.append(2 * col_half[c] + halves[4 * yh + c, row])
        depth = 16

        def body(i, carry):
            rows = pl.ds(pl.multiple_of(k * PR + i * depth, depth), depth)
            tiles = [out[c, g, rows, :].astype(jnp.float32) for c in range(4)]
            for s in range(4):
                total = jnp.zeros((depth, B), jnp.float32)
                for c in range(4):
                    total = total + jnp.where(place[c] == s, tiles[c], 0.0)
                out[s, g, rows, :] = total.astype(BF)
            return carry

        lax.fori_loop(0, PR // depth, body, 0)

    def hand_on(n):
        for what in (0, 1):
            z_wait(n, what)
            z_send(n, what + 4)

    def z_step(n):
        dx, k = Z_STEPS[n]
        slot = V_SLOT[dx]
        g = (x + dx + 4) % 4
        core_recv("X", dx, 0, k)
        core_recv("X", dx, 1, k)

        def body(r, carry):
            acc = jnp.dot(
                xbuf[g * 4 + r, pl.ds(k * PR, PR), :], vbuf[slot, r], preferred_element_type=jnp.float32
            )
            stage[r] = acc.astype(BF)
            return carry

        lax.fori_loop(0, 4, body, 0, unroll=2)
        for rel in (2, 1, 3):
            sbuf[n, rel - 1] = stage[(z + rel - shift + 4) % 4]
        for what in (0, 1, 2, 3):
            z_send(n, what)
        out[z, g, pl.ds(k * PR, PR), :] = stage[(z - shift + 4) % 4]

    def relay_of(n):
        if n >= 0:
            hand_on(n)

    for k in range(CH):
        core_recv("Y", 0, 0, k)
        make_v(0, 0, k)
    for k in range(CH):
        recv("y", "Y", 0, 1, k)
        send("+", "Y", 0, 1, k)
        send("-", "Y", 0, 1, k)
        if k == 1:
            send("-", "X", 0, 0, 0)
        if k == 2:
            send("+", "X", 0, 0, 0)
            send("+", "X", 0, 0, 1)
        if k == 3:
            for j in range(1, CH):
                send("-", "X", 0, 0, j)
                if j > 1:
                    send("+", "X", 0, 0, j)
        recv("+", "Y", -1, 0, k)
        recv("-", "Y", 1, 0, k)
        core_recv("Y", 0, 1, k)
        make_v(0, 1, k)
        if k < 3:
            for d in (1, -1):
                core_recv("Y", d, 0, k)
                make_v(d, 0, k)
    for k in range(CH):
        recv("y", "X", 0, 1, k)
        if k == 2:
            recv("-", "X", 1, 0, 0)
            send("y", "X", 1, 0, 0)
        else:
            recv("-", "Y", 1, 1, min(k, 2))
        if k == 3:
            recv("+", "X", -1, 0, 0)
            send("y", "X", -1, 0, 0)
        else:
            recv("+", "Y", -1, 1, k)
        z_step(k)
        relay_of(k - 1)
        if k == 0:
            for d in (1, -1):
                core_recv("Y", d, 0, 3)
                make_v(d, 0, 3)
        if k < 3:
            core_recv("Y", -1, 1, k)
            make_v(-1, 1, k)
        if k != 2:
            core_recv("Y", 1, 1, min(k, 2))
            make_v(1, 1, min(k, 2))
    for u in range(8, 19):
        if u == 8:
            recv("-", "Y", 1, 1, 3)
            recv("+", "X", -1, 0, 1)
            send("y", "X", -1, 0, 1)
            for d, sign, a, b in ((-1, "+", 0, 1), (1, "-", 2, 3)):
                send(sign, "Y", d, 0, a)
                send(sign, "Y", d, 0, b)
            send("+", "X", -1, 0, 1)
            send("+", "Y", -1, 1, 0)
        elif u <= 11:
            k = u - 8
            recv("-", "X", 1, 0, k)
            send("y", "X", 1, 0, k)
            if k == 1:
                recv("+", "Y", -1, 1, 3)
                send("+", "Y", -1, 1, 1)
                send("+", "X", -1, 0, 0)
            else:
                recv("+", "X", -1, 0, k)
                send("y", "X", -1, 0, k)
            if k == 3:
                send("-", "X", 1, 0, 3)
                send("-", "Y", 1, 1, 2)
                send("-", "Y", 1, 1, 3)
                send("-", "X", 1, 0, 2)
        elif u <= 13:
            recv("+", "Y", 2, 0, u - 12)
            recv("-", "Y", 2, 0, u - 10)
        elif u == 14:
            recv("+", "X", 2, 0, 1)
            send("y", "X", 2, 0, 1)
            recv("-", "X", 2, 0, 3)
            send("y", "X", 2, 0, 3)
        elif u <= 16:
            recv("+", "Y", 2, 1, u - 15)
            recv("-", "Y", 2, 1, u - 13)
        elif u == 17:
            recv("+", "X", 2, 0, 0)
            recv("-", "X", 2, 0, 2)
        else:
            recv("+", "X", 2, 1, 0)
            recv("-", "X", 2, 1, 2)
        if u < 16:
            d, k = Z_STEPS[u - 4]
            recv("y", "X", d, 1, k)
            if (d, k) == (-1, 0):
                send("+", "X", -1, 1, 0)
            if (d, k) == (1, 2):
                send("-", "X", 1, 1, 2)
        elif u < 18:
            recv("y", "X", 2, 1, 1 if u == 16 else 3)
        if u == 8:
            core_recv("Y", 1, 1, 3)
            make_v(1, 1, 3)
        if u == 9:
            core_recv("Y", -1, 1, 3)
            make_v(-1, 1, 3)
        if u == 16:
            for k in (1, 3):
                core_recv("Y", 2, 1, k)
                make_v(2, 1, k)
        z_step(u - 4)
        if u < 18:
            relay_of(u - 5)
            sum_step(u - 8)
        if u in (12, 13):
            for k in (0, 2) if u == 12 else (1, 3):
                core_recv("Y", 2, 0, k)
                make_v(2, 0, k)
        if u == 15:
            for k in (0, 2):
                core_recv("Y", 2, 1, k)
                make_v(2, 1, k)
    z_step(4 * CH - 1)
    for n in (13, 14, 15):
        hand_on(n)
        sum_step(n - 3)
    for n in (13, 14, 15):
        sum_step(n)
    copy_of(xbuf.at[pl.ds(0, len(LINK_OPS) // CH)], ls, lr.at[0], "y").wait_send()
    copy_of(xbuf, cs, cr.at[0], "c").wait_send()
    copy_of(out, zs, zlast.at[0], "z+").wait_send()


def main_call(xin, yin, pin, qin, lrank, urank, halves, shifts):
    hbm = pl.BlockSpec(memory_space=pl.ANY)
    smem = pl.BlockSpec(memory_space=pltpu.SMEM)
    steps = 4 * CH
    return pl.pallas_call(
        main_kernel,
        out_shape=pltpu.VMEM((4, 4, B, B), BF),
        in_specs=[smem] * 4 + [hbm] * 4,
        out_specs=pl.BlockSpec(memory_space=pltpu.VMEM),
        scratch_shapes=[
            pltpu.VMEM((16, B, K), BF),
            pltpu.VMEM((16, K, B), BF),
            pltpu.VMEM((3, 4, K, B), BF),
            pltpu.VMEM((B, K), BF),
            pltpu.VMEM((K, B), BF),
            pltpu.VMEM((4, PR, B), BF),
            pltpu.VMEM((steps, 3, PR, B), BF),
            pltpu.VMEM((steps, 2, HR, B), BF),
            pltpu.SemaphoreType.DMA((2 * CH + 2,)),
            pltpu.SemaphoreType.DMA,
            pltpu.SemaphoreType.DMA((len(LINK_OPS),)),
            pltpu.SemaphoreType.DMA,
            pltpu.SemaphoreType.DMA((len(CORE_OPS),)),
            pltpu.SemaphoreType.DMA,
            pltpu.SemaphoreType.DMA((steps, 2)),
            pltpu.SemaphoreType.DMA((steps,)),
        ],
        compiler_params=pltpu.CompilerParams(
            collective_id=0, has_side_effects=True, vmem_limit_bytes=58_000_000
        ),
        name="gather_update_exchange",
    )(lrank, urank, halves, shifts, xin, yin, pin, qin)


def per_device(lower_basis, lower_coeff, upper_basis, upper_coeff, lower_rank, upper_rank, child_half, owner_shift):
    blocks = main_call(
        lower_basis[0, 0], lower_coeff[0, 0], upper_basis[0, 0], upper_coeff[0, 0],
        lower_rank[0, 0], upper_rank[0, 0], child_half, owner_shift,
    )
    return blocks.reshape(1, 1, 16 * B, B)


def solution(mesh):
    whole = P("front", "tile", None, None)
    ranks = P("front", "tile", None)
    return jax.shard_map(
        per_device,
        mesh=mesh,
        in_specs=(whole, whole, whole, whole, ranks, ranks, P(), P()),
        out_specs=whole,
        check_vma=False,
    )
```

```python
import functools

import jax
import jax.numpy as jnp
from jax import lax
from jax.experimental import pallas as pl
from jax.experimental.pallas import tpu as pltpu
from jax.sharding import PartitionSpec as P

MESH = pl.DeviceIdType.MESH
B = 512
R = 32
KP = 32
K = 1024
CH = 4
PR = B // CH
SR = PR // 2
HR = SR // 2
PK = K // CH
BF = jnp.bfloat16

ALL = 20


def halves_of(k):
    return (10 + 2 * k, 11 + 2 * k)


def rows_of(k):
    if k == ALL:
        return 0, B
    return ((k - 10) * SR, SR) if k >= 10 else (k * PR, PR)


Y_OPS = (
    [("Y", 0, 0, k) for k in range(CH)]
    + [("X", 0, 0, 10 + k) for k in range(2 * CH)]
    + [("X", d, 0, 10 + k) for d in (1, -1) for k in range(2 * CH)]
    + [("X", 2, 0, h) for k in (1, 3) for h in halves_of(k)]
)


def x_ops(sign):
    a, b = (0, 1) if sign > 0 else (2, 3)
    return (
        [("Y", 0, 0, k) for k in range(CH)]
        + [("Y", 0, 1, k) for k in range(CH)]
        + [("X", 0, 0, k) for k in range(CH)]
        + [("Y", -sign, 0, a), ("Y", -sign, 0, b), ("X", -sign, 0, b)]
        + [("Y", -sign, 1, a), ("Y", -sign, 1, b), ("X", -sign, 0, a), ("X", -sign, 1, a)]
    )


LINK_OPS = [("y",) + op for op in Y_OPS] + [("+",) + op for op in x_ops(1)] + [("-",) + op for op in x_ops(-1)]
LINK_ID = {op: i for i, op in enumerate(LINK_OPS)}
CORE_OPS = (
    [("Y", dx, dy, k) for dx in (0, 1, -1, 2) for dy in (0, 1) for k in range(CH)]
    + [("X", 0, 0, ALL)]
    + [("X", dx, 1, 10 + k) for dx in (0, 1, -1) for k in range(2 * CH)]
    + [("X", dx, 0, k) for dx in (1, -1, 2) for k in range(CH)]
    + [("X", 2, 1, k) for k in (0, 2) + halves_of(1) + halves_of(3)]
)
CORE_ID = {op: i for i, op in enumerate(CORE_OPS)}
Z_PAIRS = (
    [(0, k) for k in range(CH)]
    + [(1, 0), (-1, 0), (-1, 1), (1, 1), (1, 2), (-1, 2), (1, 3), (-1, 3)]
    + [(2, k) for k in (1, 3, 0, 2)]
)
V_SLOT = {0: 0, 1: 1, -1: 2, 2: 0}


def main_kernel(
    lrank, urank, halves, shifts, xin, yin, pin, qin, out,
    xbuf, ybuf, vbuf, pbuf, qtbuf, stage, sbuf, relay,
    in_sem, ls, lr, cs, cr, zs, zr, zlast,
):
    front, tile = lax.axis_index("front"), lax.axis_index("tile")
    yh, z = front // 4, front % 4
    x, yl, core = tile // 4, (tile // 2) % 2, tile % 2

    def tile_at(gx, gy, gc):
        return (gx * 2 + gy) * 2 + gc

    dev = {
        "y": (front, tile_at(x, 1 - yl, core)),
        "+": (front, tile_at((x + 1) % 4, yl, core)),
        "-": (front, tile_at((x + 3) % 4, yl, core)),
        "c": (front, tile_at(x, yl, 1 - core)),
        "z+": (yh * 4 + (z + 1) % 4, tile),
        "z-": (yh * 4 + (z + 3) % 4, tile),
    }

    def row_of(dx, dy, gc):
        gy = yl if dy == 0 else 1 - yl
        return tile_at((x + dx + 4) % 4, gy, gc)

    def piece(kind, dx, dy, gc, k):
        if kind == "X":
            return xbuf.at[row_of(dx, dy, gc), pl.ds(*rows_of(k)), :]
        return ybuf.at[row_of(dx, dy, gc), pl.ds(k * PK, PK), :]

    def copy_of(ref, ssem, rsem, to):
        return pltpu.make_async_remote_copy(
            src_ref=ref, dst_ref=ref, send_sem=ssem, recv_sem=rsem,
            device_id=dev[to], device_id_type=MESH,
        )

    def send(link, kind, dx, dy, k):
        i = LINK_ID[(link, kind, dx, dy, k)]
        copy_of(piece(kind, dx, dy, core, k), ls, lr.at[i], link).start()

    def core_send(kind, dx, dy, k):
        i = CORE_ID[(kind, dx, dy, k)]
        copy_of(piece(kind, dx, dy, core, k), cs, cr.at[i], "c").start()

    def core_recv(kind, dx, dy, k):
        i = CORE_ID[(kind, dx, dy, k)]
        copy = copy_of(piece(kind, dx, dy, 1 - core, k), cs, cr.at[i], "c")
        copy.wait_recv()

    def recv(link, kind, dx, dy, k):
        if link == "y":
            sender = (kind, dx, 1 - dy, k)
        elif link == "+":
            sender = (kind, (dx + 2) % 4 - 1, dy, k)
        else:
            sender = (kind, dx % 4 - 1, dy, k)
        i = LINK_ID[(link,) + sender]
        copy = copy_of(piece(kind, dx, dy, core, k), ls, lr.at[i], link)
        copy.wait_recv()
        core_send(kind, dx, dy, k)

    me = tile

    def raw(n, k):
        return vbuf.at[2, n, pl.ds(k // 2 * B, B), pl.ds(k % 2 * PK, PK)]

    y_loads = []
    for k in range(CH):
        cols = pl.ds(k * PK, PK)
        copy = pltpu.make_async_copy(yin.at[:, cols], raw(0, k), in_sem.at[k])
        copy.start()
        y_loads.append(copy)
    x_load = pltpu.make_async_copy(xin, xbuf.at[me], in_sem.at[CH])
    p_load = pltpu.make_async_copy(pin, pbuf, in_sem.at[CH + 1])
    q_loads = [
        pltpu.make_async_copy(qin.at[:, pl.ds(k * PK, PK)], raw(1, k), in_sem.at[CH + 2 + k])
        for k in range(CH)
    ]
    for copy in [x_load, p_load] + q_loads:
        copy.start()

    barrier = pltpu.get_barrier_semaphore()
    for name in ("y", "+", "-", "c", "z+", "z-"):
        pl.semaphore_signal(barrier, inc=1, device_id=dev[name], device_id_type=MESH)

    col = lax.broadcasted_iota(jnp.int32, (8, K), 1)

    def keep(ranks):
        limit = jnp.zeros((8, K), jnp.int32)
        for k in range(KP):
            limit = jnp.where(col // R == k, ranks[k], limit)
        return (col % R < limit).astype(jnp.float32)[:1]

    lkeep = keep(lrank)

    def turn_y(k):
        y_loads[k].wait()
        part = raw(0, k)[...].astype(jnp.float32) * lkeep[:, k * PK : (k + 1) * PK]
        ybuf[me, k * PK : (k + 1) * PK, :] = part.T.astype(BF)

    def send_own_y(k):
        for link in ("y", "+", "-"):
            send(link, "Y", 0, 0, k)
        core_send("Y", 0, 0, k)

    turn_y(0)
    turn_y(1)
    pl.semaphore_wait(barrier, 6)
    for k in range(CH):
        send_own_y(k)
        if k + 2 < CH:
            turn_y(k + 2)
    x_load.wait()
    for k in range(2 * CH):
        send("y", "X", 0, 0, 10 + k)
    core_send("X", 0, 0, ALL)

    ukeep = keep(urank)
    p_load.wait()
    pbuf[...] = (pbuf[...].astype(jnp.float32) * ukeep).astype(BF)
    for k in range(CH):
        q_loads[k].wait()
        qtbuf[k * PK : (k + 1) * PK, :] = raw(1, k)[...].astype(jnp.float32).T.astype(BF)

    def make_v(dx, dy, k, classes=(0, 1)):
        slot = V_SLOT[dx]
        gy = yl if dy == 0 else 1 - yl
        rows = slice(k * PK, (k + 1) * PK)
        same = (
            lax.broadcasted_iota(jnp.int32, (PK, PK), 0) // R
            == lax.broadcasted_iota(jnp.int32, (PK, PK), 1) // R
        )
        cores = [core if c == 0 else 1 - core for c in classes]
        middles = []
        for gc in cores:
            m = jnp.dot(
                ybuf[row_of(dx, dy, gc), rows, :], pbuf[:, rows], preferred_element_type=jnp.float32
            )
            middles.append(jnp.where(same, m, 0.0).astype(BF))
        for gc, m in zip(cores, middles):
            v = jnp.dot(m, qtbuf[rows, :], preferred_element_type=jnp.float32)
            vbuf[slot, gy * 2 + gc, rows, :] = v.astype(BF)

    col_half = [halves[4 * yh + c, tile] for c in range(4)]
    col_shift = [shifts[yh, tile + 16 * col_half[c]] for c in range(4)]
    half = halves[front, tile]
    shift = shifts[yh, tile + 16 * half]

    def z_copy(n, what, src, dst, to):
        return pltpu.make_async_remote_copy(
            src_ref=src, dst_ref=dst, send_sem=zs, recv_sem=zr.at[n] if what < 2 else zlast.at[n // 2],
            device_id=dev[to], device_id_type=MESH,
        )

    def z_place(n):
        dx, k = Z_PAIRS[n // 2]
        return dx, (x + dx + 4) % 4, 2 * k + n % 2

    def z_refs(n, what):
        _, g, kk = z_place(n)
        row = kk * SR
        if what == 0:
            return sbuf.at[n, 1, pl.ds(0, HR), :], relay.at[n, 0], "z+"
        if what == 1:
            return sbuf.at[n, 1, pl.ds(HR, HR), :], relay.at[n, 1], "z-"
        if what == 2:
            return sbuf.at[n, 0], out.at[z, g, pl.ds(row, SR), :], "z+"
        if what == 3:
            return sbuf.at[n, 2], out.at[z, g, pl.ds(row, SR), :], "z-"
        if what == 4:
            return relay.at[n, 0], out.at[(z + 3) % 4, g, pl.ds(row, HR), :], "z+"
        return relay.at[n, 1], out.at[(z + 1) % 4, g, pl.ds(row + HR, HR), :], "z-"

    def z_send(n, what):
        src, dst, to = z_refs(n, what)
        z_copy(n, what, src, dst, to).start()

    def sum_step(n):
        dx, k = Z_PAIRS[n]
        g = (x + dx + 4) % 4
        theirs = out.at[pl.ds(0, 3), g, pl.ds(k * PR, PR), :]
        copy = z_copy(2 * n, 2, theirs, theirs, "z+")
        copy.wait_recv()
        place = []
        for c in range(4):
            row = 4 * g + (z - col_shift[c] + 4) % 4
            place.append(2 * col_half[c] + halves[4 * yh + c, row])
        depth = 16

        def body(i, carry):
            rows = pl.ds(pl.multiple_of(k * PR + i * depth, depth), depth)
            tiles = [out[c, g, rows, :].astype(jnp.float32) for c in range(4)]
            for s in range(4):
                total = jnp.zeros((depth, B), jnp.float32)
                for c in range(4):
                    total = total + jnp.where(place[c] == s, tiles[c], 0.0)
                out[s, g, rows, :] = total.astype(BF)
            return carry

        lax.fori_loop(0, PR // depth, body, 0)

    def hand_on(n):
        copy = z_copy(n, 0, relay.at[n], relay.at[n], "z+")
        copy.wait_recv()
        for what in (4, 5):
            z_send(n, what)

    def z_step(n):
        dx, g, kk = z_place(n)
        slot = V_SLOT[dx]

        def tiles_of(gc):
            for gy in range(2):
                r = 2 * gy + gc
                acc = jnp.dot(
                    xbuf[g * 4 + r, pl.ds(kk * SR, SR), :], vbuf[slot, r], preferred_element_type=jnp.float32
                )
                stage[r] = acc.astype(BF)

        tiles_of(core)
        if dx == 0:
            if kk == 0:
                core_recv("X", 0, 0, ALL)
        elif kk % 2 == 0:
            core_recv("X", dx, 0, kk // 2)
        if dx != 2 or kk // 2 in (1, 3):
            core_recv("X", dx, 1, 10 + kk)
        elif kk % 2 == 0:
            core_recv("X", dx, 1, kk // 2)
        tiles_of(1 - core)
        for rel in (2, 1, 3):
            sbuf[n, rel - 1] = stage[(z + rel - shift + 4) % 4]
        for what in (0, 1, 2, 3):
            z_send(n, what)
        out[z, g, pl.ds(kk * SR, SR), :] = stage[(z - shift + 4) % 4]

    def relay_of(n):
        if n >= 0:
            hand_on(n)

    for k in range(CH):
        core_recv("Y", 0, 0, k)
        make_v(0, 0, k)
    for k in range(CH):
        recv("y", "Y", 0, 1, k)
        send("+", "Y", 0, 1, k)
        send("-", "Y", 0, 1, k)
        if k == 1:
            send("-", "X", 0, 0, 0)
        if k == 2:
            send("+", "X", 0, 0, 0)
            send("+", "X", 0, 0, 1)
        if k == 3:
            for j in range(1, CH):
                send("-", "X", 0, 0, j)
                if j > 1:
                    send("+", "X", 0, 0, j)
        recv("+", "Y", -1, 0, k)
        recv("-", "Y", 1, 0, k)
        core_recv("Y", 0, 1, k)
        make_v(0, 1, k)
        if k < 3:
            for d in (1, -1):
                core_recv("Y", d, 0, k)
                make_v(d, 0, k)
    for k in range(CH):
        recv("y", "X", 0, 1, 10 + 2 * k)
        z_step(2 * k)
        relay_of(2 * k - 1)
        if k == 0:
            for d in (1, -1):
                core_recv("Y", d, 0, 3)
                make_v(d, 0, 3)
        recv("y", "X", 0, 1, 11 + 2 * k)
        if k == 2:
            recv("-", "X", 1, 0, 0)
            for h in halves_of(0):
                send("y", "X", 1, 0, h)
        else:
            recv("-", "Y", 1, 1, min(k, 2))
        if k == 3:
            recv("+", "X", -1, 0, 0)
            for h in halves_of(0):
                send("y", "X", -1, 0, h)
        else:
            recv("+", "Y", -1, 1, k)
        z_step(2 * k + 1)
        relay_of(2 * k)
        if k < 3:
            core_recv("Y", -1, 1, k)
            make_v(-1, 1, k)
        if k != 2:
            core_recv("Y", 1, 1, min(k, 2))
            make_v(1, 1, min(k, 2))
    for u in range(8, 19):
        pair = u - 4
        d, k = Z_PAIRS[pair]
        if u < 18:
            if u == 8:
                recv("-", "Y", 1, 1, 3)
            if u == 16:
                recv("+", "Y", 2, 1, 1)
                recv("-", "Y", 2, 1, 3)
            recv("y", "X", d, 1, 10 + 2 * k)
            if u == 8:
                core_recv("Y", 1, 1, 3)
                make_v(1, 1, 3)
            if u == 9:
                recv("+", "Y", -1, 1, 3)
                core_recv("Y", -1, 1, 3)
                make_v(-1, 1, 3)
            if u == 16:
                for j in (1, 3):
                    core_recv("Y", 2, 1, j)
                    make_v(2, 1, j)
            z_step(2 * pair)
            relay_of(2 * pair - 1)
        if u < 18:
            recv("y", "X", d, 1, 11 + 2 * k)
        if u == 8:
            recv("+", "X", -1, 0, 1)
            for h in halves_of(1):
                send("y", "X", -1, 0, h)
            for e, sign, a, b in ((-1, "+", 0, 1), (1, "-", 2, 3)):
                send(sign, "Y", e, 0, a)
                send(sign, "Y", e, 0, b)
            send("+", "X", -1, 0, 1)
            send("+", "Y", -1, 1, 0)
        elif u <= 11:
            j = u - 8
            recv("-", "X", 1, 0, j)
            for h in halves_of(j):
                send("y", "X", 1, 0, h)
            if j == 1:
                send("+", "Y", -1, 1, 1)
                send("+", "X", -1, 0, 0)
                send("+", "X", -1, 1, 0)
            else:
                recv("+", "X", -1, 0, j)
                for h in halves_of(j):
                    send("y", "X", -1, 0, h)
            if j == 3:
                send("-", "X", 1, 0, 3)
                send("-", "Y", 1, 1, 2)
                send("-", "Y", 1, 1, 3)
                send("-", "X", 1, 0, 2)
        elif u <= 13:
            recv("+", "Y", 2, 0, u - 12)
            recv("-", "Y", 2, 0, u - 10)
        elif u == 14:
            recv("+", "X", 2, 0, 1)
            for h in halves_of(1):
                send("y", "X", 2, 0, h)
            recv("-", "X", 2, 0, 3)
            for h in halves_of(3):
                send("y", "X", 2, 0, h)
        elif u == 15:
            recv("+", "Y", 2, 1, 0)
            recv("-", "Y", 2, 1, 2)
        elif u == 17:
            recv("+", "X", 2, 0, 0)
            recv("-", "X", 2, 0, 2)
        elif u == 18:
            recv("+", "X", 2, 1, 0)
            recv("-", "X", 2, 1, 2)
        if (d, k) == (1, 2):
            send("-", "X", 1, 1, 2)
        if u < 18:
            z_step(2 * pair + 1)
            relay_of(2 * pair)
            sum_step(pair - 4)
        if u in (12, 13):
            for j in (0, 2) if u == 12 else (1, 3):
                core_recv("Y", 2, 0, j)
                make_v(2, 0, j)
        if u == 15:
            for j in (0, 2):
                core_recv("Y", 2, 1, j)
                make_v(2, 1, j)
    for n in range(28, 32):
        z_step(n)
        relay_of(n - 1)
    hand_on(31)
    for n in range(10, 16):
        sum_step(n)
    copy_of(xbuf.at[pl.ds(0, 14)], ls, lr.at[0], "y").wait_send()
    copy_of(xbuf, cs, cr.at[0], "c").wait_send()
    copy_of(out, zs, zlast.at[0], "z+").wait_send()


def main_call(xin, yin, pin, qin, lrank, urank, halves, shifts):
    hbm = pl.BlockSpec(memory_space=pl.ANY)
    smem = pl.BlockSpec(memory_space=pltpu.SMEM)
    steps = 8 * CH
    return pl.pallas_call(
        main_kernel,
        out_shape=pltpu.VMEM((4, 4, B, B), BF),
        in_specs=[smem] * 4 + [hbm] * 4,
        out_specs=pl.BlockSpec(memory_space=pltpu.VMEM),
        scratch_shapes=[
            pltpu.VMEM((16, B, K), BF),
            pltpu.VMEM((16, K, B), BF),
            pltpu.VMEM((3, 4, K, B), BF),
            pltpu.VMEM((B, K), BF),
            pltpu.VMEM((K, B), BF),
            pltpu.VMEM((4, SR, B), BF),
            pltpu.VMEM((steps, 3, SR, B), BF),
            pltpu.VMEM((steps, 2, HR, B), BF),
            pltpu.SemaphoreType.DMA((2 * CH + 2,)),
            pltpu.SemaphoreType.DMA,
            pltpu.SemaphoreType.DMA((len(LINK_OPS),)),
            pltpu.SemaphoreType.DMA,
            pltpu.SemaphoreType.DMA((len(CORE_OPS),)),
            pltpu.SemaphoreType.DMA,
            pltpu.SemaphoreType.DMA((steps,)),
            pltpu.SemaphoreType.DMA((steps // 2,)),
        ],
        compiler_params=pltpu.CompilerParams(
            collective_id=0, has_side_effects=True, vmem_limit_bytes=58_000_000
        ),
        name="gather_update_exchange",
    )(lrank, urank, halves, shifts, xin, yin, pin, qin)


def per_device(lower_basis, lower_coeff, upper_basis, upper_coeff, lower_rank, upper_rank, child_half, owner_shift):
    blocks = main_call(
        lower_basis[0, 0], lower_coeff[0, 0], upper_basis[0, 0], upper_coeff[0, 0],
        lower_rank[0, 0], upper_rank[0, 0], child_half, owner_shift,
    )
    return blocks.reshape(1, 1, 16 * B, B)


def solution(mesh):
    whole = P("front", "tile", None, None)
    ranks = P("front", "tile", None)
    return jax.shard_map(
        per_device,
        mesh=mesh,
        in_specs=(whole, whole, whole, whole, ranks, ranks, P(), P()),
        out_specs=whole,
        check_vma=False,
    )
```

```python
import functools

import jax
import jax.numpy as jnp
from jax import lax
from jax.experimental import pallas as pl
from jax.experimental.pallas import tpu as pltpu
from jax.sharding import PartitionSpec as P

MESH = pl.DeviceIdType.MESH
B = 512
R = 32
KP = 32
K = 1024
CH = 4
PR = B // CH
PK = K // CH
BF = jnp.bfloat16
F32 = jnp.float32


def piece_rows(k):
    return (k * PR, PR)


FULL = (0, B)
HALVES = [(i * PR // 2, PR // 2) for i in range(2 * CH)]

Y_OPS = (
    [("Y", 0, 0, k) for k in range(CH)]
    + [("X", 0, 0, h) for h in HALVES]
    + [("X", d, 0, piece_rows(k)) for k in range(1, CH) for d in (1, -1)]
)


def x_ops(sign):
    a, b = (0, 1) if sign > 0 else (2, 3)
    return (
        [("P", 0, 0, q) for q in range(CH)]
        + [("P", -sign, 0, a), ("P", -sign, 0, b)]
        + [("X", 0, 0, piece_rows(k)) for k in range(CH)]
        + [("X", 0, 1, piece_rows(0))]
        + [("X", -sign, dy, piece_rows(k)) for dy in (0, 1) for k in (a, b)]
        + [("M", sign, 0, 0), ("M", 2, 0, 0), ("M", 2, 0, 1)]
    )


LINK_OPS = [("y",) + op for op in Y_OPS] + [("+",) + op for op in x_ops(1)] + [("-",) + op for op in x_ops(-1)]
LINK_ID = {op: i for i, op in enumerate(LINK_OPS)}
CORE_OPS = (
    [("Y", 0, dy, k) for dy in (0, 1) for k in range(CH)]
    + [("X", 0, 0, FULL)]
    + [("X", 0, 1, h) for h in HALVES]
    + [("X", dx, dy, piece_rows(k)) for dx in (1, -1, 2) for dy in (0, 1) for k in range(CH)]
)
CORE_ID = {op: i for i, op in enumerate(CORE_OPS)}
Z_STEPS = (
    [(0, h) for h in HALVES]
    + [(d, piece_rows(k)) for k in range(CH) for d in (1, -1)]
    + [(2, piece_rows(k)) for k in (0, 2, 1, 3)]
)
SUMS = [(0, k) for k in range(CH)] + [(dx, row // PR) for dx, (row, _) in Z_STEPS[2 * CH :]]
Z_AT = [sum(rows for _, (_, rows) in Z_STEPS[:n]) for n in range(len(Z_STEPS))]
SLOT = {0: 0, 1: 1, -1: 2, 2: 3}


def main_kernel(
    lrank, urank, halves, shifts, xin, yin, pin, qin, out,
    xbuf, ybuf, vbuf, pbuf, mout, minto, mrel, qtbuf, stage, sbuf, relay,
    in_sem, ls, lr, cs, cr, zs, zr, zlast,
):
    front, tile = lax.axis_index("front"), lax.axis_index("tile")
    yh, z = front // 4, front % 4
    x, yl, core = tile // 4, (tile // 2) % 2, tile % 2

    def tile_at(gx, gy, gc):
        return (gx * 2 + gy) * 2 + gc

    dev = {
        "y": (front, tile_at(x, 1 - yl, core)),
        "+": (front, tile_at((x + 1) % 4, yl, core)),
        "-": (front, tile_at((x + 3) % 4, yl, core)),
        "c": (front, tile_at(x, yl, 1 - core)),
        "z+": (yh * 4 + (z + 1) % 4, tile),
        "z-": (yh * 4 + (z + 3) % 4, tile),
    }

    def row_of(dx, dy, gc):
        gy = yl if dy == 0 else 1 - yl
        return tile_at((x + dx + 4) % 4, gy, gc)

    def piece(kind, dx, dy, gc, k):
        if kind == "X":
            return xbuf.at[row_of(dx, dy, gc), pl.ds(*k), :]
        gy = yl if dy == 0 else 1 - yl
        return ybuf.at[2 * gy + gc, pl.ds(k * PK, PK), :]

    def copy_of(src, dst, ssem, rsem, to):
        return pltpu.make_async_remote_copy(
            src_ref=src, dst_ref=dst, send_sem=ssem, recv_sem=rsem,
            device_id=dev[to], device_id_type=MESH,
        )

    def send(link, kind, dx, dy, k):
        i = LINK_ID[(link, kind, dx, dy, k)]
        sign = 1 if link == "+" else -1
        if kind == "P":
            src = pbuf.at[SLOT[dx], k]
            dst = pbuf.at[SLOT[-sign] if dx == 0 else SLOT[2], k]
        elif kind == "M":
            part = pl.ds(0 if sign > 0 else 2, 2)
            if dx == sign:
                src, dst = mout.at[SLOT[sign] - 1], minto.at[SLOT[-sign] - 1]
            elif k == 0:
                src, dst = mout.at[SLOT[2] - 1, part], mrel.at[0 if sign > 0 else 1]
            else:
                src, dst = mrel.at[0 if sign > 0 else 1], minto.at[SLOT[2] - 1, part]
        else:
            src = dst = piece(kind, dx, dy, core, k)
        copy_of(src, dst, ls, lr.at[i], link).start()

    def core_send(kind, dx, dy, k):
        i = CORE_ID[(kind, dx, dy, k)]
        ref = piece(kind, dx, dy, core, k)
        copy_of(ref, ref, cs, cr.at[i], "c").start()

    def core_recv(kind, dx, dy, k):
        i = CORE_ID[(kind, dx, dy, k)]
        ref = piece(kind, dx, dy, 1 - core, k)
        copy = copy_of(ref, ref, cs, cr.at[i], "c")
        copy.wait_recv()

    def await_link(link, sender, ref):
        copy = copy_of(ref, ref, ls, lr.at[LINK_ID[(link,) + sender]], link)
        copy.wait_recv()

    def recv(link, kind, dx, dy, k):
        if link == "y":
            sender = (kind, dx, 1 - dy, k)
        elif link == "+":
            sender = (kind, (dx + 2) % 4 - 1, dy, k)
        else:
            sender = (kind, dx % 4 - 1, dy, k)
        await_link(link, sender, piece(kind, dx, dy, core, k))
        core_send(kind, dx, dy, k)

    def recv_p(dx, q):
        if dx == 2:
            sign = 1 if q < 2 else -1
            sender = ("P", -sign, 0, q)
        else:
            sign = -dx
            sender = ("P", 0, 0, q)
        await_link("+" if sign > 0 else "-", sender, pbuf.at[SLOT[dx], q])

    me = tile

    def raw(n, k):
        return vbuf.at[3, n, pl.ds(k // 2 * B, B), pl.ds(k % 2 * PK, PK)]

    def columns(ref, k):
        return ref.at[:, pl.ds(k * PK, PK)]

    y_loads, p_loads, q_loads = [], [], []
    for k in range(CH):
        y_loads.append(pltpu.make_async_copy(columns(yin, k), raw(0, k), in_sem.at[k]))
        p_loads.append(pltpu.make_async_copy(columns(pin, k), pbuf.at[0, k], in_sem.at[CH + k]))
        q_loads.append(pltpu.make_async_copy(columns(qin, k), raw(1, k), in_sem.at[2 * CH + k]))
    x_load = pltpu.make_async_copy(xin, xbuf.at[me], in_sem.at[3 * CH])
    for copy in y_loads + p_loads + [x_load] + q_loads:
        copy.start()

    barrier = pltpu.get_barrier_semaphore()
    for name in ("y", "+", "-", "c", "z+", "z-"):
        pl.semaphore_signal(barrier, inc=1, device_id=dev[name], device_id_type=MESH)

    col = lax.broadcasted_iota(jnp.int32, (8, K), 1)

    def keep(ranks):
        limit = jnp.zeros((8, K), jnp.int32)
        for k in range(KP):
            limit = jnp.where(col // R == k, ranks[k], limit)
        return (col % R < limit).astype(F32)[:1]

    lkeep = keep(lrank)
    ukeep = keep(urank)

    def ready(k):
        cols = slice(k * PK, (k + 1) * PK)
        y_loads[k].wait()
        part = raw(0, k)[...].astype(F32) * lkeep[:, cols]
        ybuf[2 * yl + core, cols, :] = part.T.astype(BF)
        p_loads[k].wait()
        pbuf[0, k] = (pbuf[0, k].astype(F32) * ukeep[:, cols]).astype(BF)

    ready(0)
    pl.semaphore_wait(barrier, 6)
    for k in range(CH):
        if k + 1 < CH:
            ready(k + 1)
        send("y", "Y", 0, 0, k)
        core_send("Y", 0, 0, k)
        send("+", "P", 0, 0, k)
        send("-", "P", 0, 0, k)
    x_load.wait()
    for h in HALVES:
        send("y", "X", 0, 0, h)
    core_send("X", 0, 0, FULL)
    for k in range(CH):
        q_loads[k].wait()
        qtbuf[k * PK : (k + 1) * PK, :] = raw(1, k)[...].astype(F32).T.astype(BF)

    def same_panel():
        a = lax.broadcasted_iota(jnp.int32, (PK, PK), 0) // R
        return a == lax.broadcasted_iota(jnp.int32, (PK, PK), 1) // R

    def middle(r, slot, q):
        rows = slice(q * PK, (q + 1) * PK)
        m = jnp.dot(ybuf[r, rows, :], pbuf[slot, q], preferred_element_type=F32)
        return jnp.where(same_panel(), m, 0.0)

    def put_v(slot, rs, q, middles):
        rows = slice(q * PK, (q + 1) * PK)
        for r, m in zip(rs, middles):
            v = jnp.dot(m, qtbuf[rows, :], preferred_element_type=F32)
            vbuf[slot, r, rows, :] = v.astype(BF)

    def own_v(dy, k, classes=(0, 1)):
        gy = yl if dy == 0 else 1 - yl
        rs = [2 * gy + (core if c == 0 else 1 - core) for c in classes]
        put_v(0, rs, k, [middle(r, 0, k).astype(BF) for r in rs])

    def make_m(dx, q):
        for r in range(4):
            m = middle(r, SLOT[dx], q)
            m = m[:, : PK // 2] + m[:, PK // 2 :]
            for t in range(2):
                part = [m[t * 128 + i * R : t * 128 + (i + 1) * R] for i in range(4)]
                mout[SLOT[dx] - 1, q, r, t * R : (t + 1) * R, :] = (part[0] + part[1] + part[2] + part[3]).astype(BF)

    def far_v(dx, q):
        middles = []
        for r in range(4):
            m = minto[SLOT[dx] - 1, q, r].astype(F32)
            m = jnp.concatenate([m[:R]] * 4 + [m[R:]] * 4, axis=0)
            m = jnp.concatenate([m, m], axis=1)
            middles.append(jnp.where(same_panel(), m, 0.0).astype(BF))
        put_v(SLOT[dx], range(4), q, middles)

    col_half = [halves[4 * yh + c, tile] for c in range(4)]
    col_shift = [shifts[yh, tile + 16 * col_half[c]] for c in range(4)]
    half = halves[front, tile]
    shift = shifts[yh, tile + 16 * half]

    def sum_of(n):
        dx, (row, _) = Z_STEPS[n]
        return SUMS.index((dx, row // PR))

    def z_copy(n, what, src, dst, to):
        rsem = zr.at[n] if what < 2 else zlast.at[sum_of(n)]
        return copy_of(src, dst, zs, rsem, to)

    def z_send(n, what):
        dx, (row, rows) = Z_STEPS[n]
        g = (x + dx + 4) % 4
        hr, at = rows // 2, Z_AT[n]
        passing = [relay.at[i, pl.ds(at // 2, hr), :] for i in range(2)]
        src, dst, to = [
            (sbuf.at[1, pl.ds(at, hr), :], passing[0], "z+"),
            (sbuf.at[1, pl.ds(at + hr, hr), :], passing[1], "z-"),
            (sbuf.at[0, pl.ds(at, rows), :], out.at[z, g, pl.ds(row, rows), :], "z+"),
            (sbuf.at[2, pl.ds(at, rows), :], out.at[z, g, pl.ds(row, rows), :], "z-"),
            (passing[0], out.at[(z + 3) % 4, g, pl.ds(row, hr), :], "z+"),
            (passing[1], out.at[(z + 1) % 4, g, pl.ds(row + hr, hr), :], "z-"),
        ][what]
        z_copy(n, what, src, dst, to).start()

    def hand_on(n):
        _, (_, rows) = Z_STEPS[n]
        both = relay.at[:, pl.ds(Z_AT[n] // 2, rows // 2), :]
        copy = z_copy(n, 0, both, both, "z+")
        copy.wait_recv()
        for what in (4, 5):
            z_send(n, what)

    handed = []

    def relay_upto(n):
        while len(handed) <= n:
            hand_on(len(handed))
            handed.append(n)

    def sum_step(n):
        dx, k = SUMS[n]
        g = (x + dx + 4) % 4
        theirs = out.at[pl.ds(0, 3), g, pl.ds(k * PR, PR), :]
        copy = copy_of(theirs, theirs, zs, zlast.at[n], "z+")
        copy.wait_recv()
        place = []
        for c in range(4):
            row = 4 * g + (z - col_shift[c] + 4) % 4
            place.append(2 * col_half[c] + halves[4 * yh + c, row])
        depth = 16

        def body(i, carry):
            rows = pl.ds(pl.multiple_of(k * PR + i * depth, depth), depth)
            tiles = [out[c, g, rows, :].astype(jnp.float32) for c in range(4)]
            for s in range(4):
                total = jnp.zeros((depth, B), jnp.float32)
                for c in range(4):
                    total = total + jnp.where(place[c] == s, tiles[c], 0.0)
                out[s, g, rows, :] = total.astype(BF)
            return carry

        lax.fori_loop(0, PR // depth, body, 0)

    pending = []

    def later(work, *args):
        pending.append(functools.partial(work, *args))

    def run_some(count):
        for _ in range(min(count, len(pending))):
            pending.pop(0)()

    def z_step(n):
        dx, (row, rows) = Z_STEPS[n]
        g = (x + dx + 4) % 4
        at = Z_AT[n]

        def tiles_of(gc):
            for gy in range(2):
                r = 2 * gy + gc
                acc = jnp.dot(
                    xbuf[g * 4 + r, pl.ds(row, rows), :], vbuf[SLOT[dx], r], preferred_element_type=F32
                )
                stage[r, :rows] = acc.astype(BF)

        tiles_of(core)
        run_some(1)
        if dx != 0:
            core_recv("X", dx, 0, (row, rows))
        elif n == 0:
            core_recv("X", 0, 0, FULL)
        core_recv("X", dx, 1, (row, rows))
        tiles_of(1 - core)
        for rel in (2, 1, 3):
            sbuf[rel - 1, at : at + rows, :] = stage[(z + rel - shift + 4) % 4, :rows]
        for what in (0, 1, 2, 3):
            z_send(n, what)
        out[z, g, row : row + rows, :] = stage[(z - shift + 4) % 4, :rows]

    def pass_on(link, dx, k):
        recv(link, "X", dx, 0, piece_rows(k))
        send("y", "X", dx, 0, piece_rows(k))

    both = (("-", 1), ("+", -1))

    for k in range(CH):
        own_v(0, k, (0,))
    for k in range(CH):
        core_recv("Y", 0, 0, k)
        own_v(0, k, (1,))
    for k in range(CH):
        recv("y", "Y", 0, 1, k)
        if k == 3:
            own_v(1, k, (0,))
        for dx in (1, -1):
            recv_p(dx, k)
        if k == 3:
            for link, _ in both:
                send(link, "X", 0, 0, piece_rows(0))
        core_recv("Y", 0, 1, k)
        own_v(1, k, (0, 1) if k < 3 else (1,))
        make_m(1, k)
        make_m(-1, k)
    send("+", "M", 1, 0, 0)
    send("-", "M", -1, 0, 0)
    for h in range(2 * CH):
        recv("y", "X", 0, 1, HALVES[h])
        if h == 1:
            for link, dx in both:
                send(link, "X", 0, 1, piece_rows(0))
                send(link, "X", 0, 0, piece_rows(1))
                for q, k in ((0, 2), (1, 3)) if link == "+" else ((2, 2), (3, 3)):
                    send(link, "P", dx, 0, q)
                    send(link, "X", 0, 0, piece_rows(k))
        z_step(h)
        relay_upto(h - 1)
        if h == 2:
            for link, dx in both:
                recv(link, "X", dx, 0, piece_rows(0))
        if h == 4:
            await_link("-", ("M", -1, 0, 0), minto.at[SLOT[1] - 1])
            await_link("+", ("M", 1, 0, 0), minto.at[SLOT[-1] - 1])
            for q in range(CH):
                later(far_v, 1, q)
            for q in range(CH):
                later(far_v, -1, q)
        if h == 5:
            for link, dx in both:
                recv(link, "X", dx, 1, piece_rows(0))
        if h == 7:
            for link, dx in both:
                pass_on(link, dx, 1)
        if h > 4:
            run_some(1)
    while pending:
        run_some(1)
    for n in range(8, 20):
        dx, (row, _) = Z_STEPS[n]
        if 10 <= n < 16:
            recv("y", "X", dx, 1, (row, PR))
        z_step(n)
        relay_upto(n - 1 if n < 17 else n - 2)
        if n in (8, 10):
            for q in (0, 2) if n == 8 else (1, 3):
                recv_p(2, q)
                make_m(2, q)
        if n == 10:
            send("+", "M", 2, 0, 0)
            send("-", "M", 2, 0, 0)
        if n in (9, 11):
            for link, e in both:
                pass_on(link, e, 2 if n == 9 else 3)
        if n == 10:
            for k in (0, 1):
                send("+", "X", -1, 0, piece_rows(k))
            send("-", "X", 1, 0, piece_rows(2))
        if n == 11:
            send("-", "X", 1, 0, piece_rows(3))
        if n == 12:
            for link, i in (("+", 0), ("-", 1)):
                await_link(link, ("M", 2, 0, 0), mrel.at[i])
                send(link, "M", 2, 0, 1)
            send("+", "X", -1, 1, piece_rows(0))
            send("+", "X", -1, 1, piece_rows(1))
            send("-", "X", 1, 1, piece_rows(2))
        if n == 13:
            recv("+", "X", 2, 0, piece_rows(0))
            recv("-", "X", 2, 0, piece_rows(2))
        if n == 14:
            send("-", "X", 1, 1, piece_rows(3))
            recv("+", "X", 2, 0, piece_rows(1))
            recv("-", "X", 2, 0, piece_rows(3))
        if n == 15:
            for link, i in (("+", 0), ("-", 2)):
                await_link(link, ("M", 2, 0, 1), minto.at[SLOT[2] - 1, pl.ds(i, 2)])
            for q in range(CH):
                far_v(2, q)
            recv("+", "X", 2, 1, piece_rows(0))
            recv("-", "X", 2, 1, piece_rows(2))
        if n == 17:
            recv("+", "X", 2, 1, piece_rows(1))
            recv("-", "X", 2, 1, piece_rows(3))
        if 10 <= n < 18:
            later(sum_step, n - 10)
    while pending:
        run_some(1)
    for n in (18, 19):
        relay_upto(n)
    for n in range(8, 16):
        sum_step(n)
    twelve, ten = xbuf.at[pl.ds(0, 12)], xbuf.at[pl.ds(0, 10)]
    copy_of(twelve, twelve, ls, lr.at[0], "y").wait_send()
    copy_of(ten, ten, cs, cr.at[0], "c").wait_send()
    copy_of(out, out, zs, zlast.at[0], "z+").wait_send()


def main_call(xin, yin, pin, qin, lrank, urank, halves, shifts):
    hbm = pl.BlockSpec(memory_space=pl.ANY)
    smem = pl.BlockSpec(memory_space=pltpu.SMEM)
    return pl.pallas_call(
        main_kernel,
        out_shape=pltpu.VMEM((4, 4, B, B), BF),
        in_specs=[smem] * 4 + [hbm] * 4,
        out_specs=pl.BlockSpec(memory_space=pltpu.VMEM),
        scratch_shapes=[
            pltpu.VMEM((16, B, K), BF),
            pltpu.VMEM((4, K, B), BF),
            pltpu.VMEM((4, 4, K, B), BF),
            pltpu.VMEM((4, CH, B, PK), BF),
            pltpu.VMEM((3, CH, 4, 2 * R, 128), BF),
            pltpu.VMEM((3, CH, 4, 2 * R, 128), BF),
            pltpu.VMEM((2, 2, 4, 2 * R, 128), BF),
            pltpu.VMEM((K, B), BF),
            pltpu.VMEM((4, PR, B), BF),
            pltpu.VMEM((3, 4 * B, B), BF),
            pltpu.VMEM((2, 2 * B, B), BF),
            pltpu.SemaphoreType.DMA((3 * CH + 1,)),
            pltpu.SemaphoreType.DMA,
            pltpu.SemaphoreType.DMA((len(LINK_OPS),)),
            pltpu.SemaphoreType.DMA,
            pltpu.SemaphoreType.DMA((len(CORE_OPS),)),
            pltpu.SemaphoreType.DMA,
            pltpu.SemaphoreType.DMA((len(Z_STEPS),)),
            pltpu.SemaphoreType.DMA((len(SUMS),)),
        ],
        compiler_params=pltpu.CompilerParams(
            collective_id=0, has_side_effects=True, vmem_limit_bytes=58_000_000
        ),
        name="gather_update_exchange",
    )(lrank, urank, halves, shifts, xin, yin, pin, qin)


def per_device(lower_basis, lower_coeff, upper_basis, upper_coeff, lower_rank, upper_rank, child_half, owner_shift):
    blocks = main_call(
        lower_basis[0, 0], lower_coeff[0, 0], upper_basis[0, 0], upper_coeff[0, 0],
        lower_rank[0, 0], upper_rank[0, 0], child_half, owner_shift,
    )
    return blocks.reshape(1, 1, 16 * B, B)


def solution(mesh):
    whole = P("front", "tile", None, None)
    ranks = P("front", "tile", None)
    return jax.shard_map(
        per_device,
        mesh=mesh,
        in_specs=(whole, whole, whole, whole, ranks, ranks, P(), P()),
        out_specs=whole,
        check_vma=False,
    )
```

```python
import functools

import jax
import jax.numpy as jnp
from jax import lax
from jax.experimental import pallas as pl
from jax.experimental.pallas import tpu as pltpu
from jax.sharding import PartitionSpec as P

MESH = pl.DeviceIdType.MESH
B = 512
R = 32
KP = 32
K = 1024
CH = 4
PR = B // CH
PK = K // CH
BF = jnp.bfloat16
F32 = jnp.float32


def piece_rows(k):
    return (k * PR, PR)


FULL = (0, B)
HALVES = [(i * PR // 2, PR // 2) for i in range(2 * CH)]

Y_OPS = (
    [("Y", 0, 0, k) for k in range(CH)]
    + [("X", 0, 0, h) for h in HALVES]
    + [("X", d, 0, piece_rows(k)) for k in range(1, CH) for d in (1, -1)]
)


def x_ops(sign):
    a, b = (0, 1) if sign > 0 else (2, 3)
    return (
        [("P", 0, 0, q) for q in range(CH)]
        + [("P", -sign, 0, a), ("P", -sign, 0, b)]
        + [("X", 0, 0, piece_rows(k)) for k in range(CH)]
        + [("X", 0, 1, piece_rows(0))]
        + [("X", -sign, dy, piece_rows(k)) for dy in (0, 1) for k in (a, b)]
        + [("M", sign, 0, 0), ("M", 2, 0, 0), ("M", 2, 0, 1)]
    )


LINK_OPS = [("y",) + op for op in Y_OPS] + [("+",) + op for op in x_ops(1)] + [("-",) + op for op in x_ops(-1)]
LINK_ID = {op: i for i, op in enumerate(LINK_OPS)}
CORE_OPS = (
    [("Y", 0, dy, k) for dy in (0, 1) for k in range(CH)]
    + [("X", 0, 0, FULL)]
    + [("X", 0, 1, h) for h in HALVES]
    + [("X", dx, dy, piece_rows(k)) for dx in (1, -1, 2) for dy in (0, 1) for k in range(CH)]
)
CORE_ID = {op: i for i, op in enumerate(CORE_OPS)}
Z_STEPS = (
    [(0, h) for h in HALVES]
    + [(d, piece_rows(k)) for k in range(CH) for d in (1, -1)]
    + [(2, piece_rows(k)) for k in (0, 2, 1, 3)]
)
SUMS = [(0, k) for k in range(CH)] + [(dx, row // PR) for dx, (row, _) in Z_STEPS[2 * CH :]]
Z_AT = [sum(rows for _, (_, rows) in Z_STEPS[:n]) for n in range(len(Z_STEPS))]
SLOT = {0: 0, 1: 1, -1: 2, 2: 3}


def main_kernel(
    lrank, urank, halves, shifts, xin, yin, pin, qin, out,
    xbuf, ybuf, vbuf, pbuf, mout, minto, mrel, qtbuf, stage, sbuf, relay,
    in_sem, ls, lr, cs, cr, zs, zr, zlast,
):
    front, tile = lax.axis_index("front"), lax.axis_index("tile")
    yh, z = front // 4, front % 4
    x, yl, core = tile // 4, (tile // 2) % 2, tile % 2

    def tile_at(gx, gy, gc):
        return (gx * 2 + gy) * 2 + gc

    dev = {
        "y": (front, tile_at(x, 1 - yl, core)),
        "+": (front, tile_at((x + 1) % 4, yl, core)),
        "-": (front, tile_at((x + 3) % 4, yl, core)),
        "c": (front, tile_at(x, yl, 1 - core)),
        "z+": (yh * 4 + (z + 1) % 4, tile),
        "z-": (yh * 4 + (z + 3) % 4, tile),
    }

    def row_of(dx, dy, gc):
        gy = yl if dy == 0 else 1 - yl
        return tile_at((x + dx + 4) % 4, gy, gc)

    def piece(kind, dx, dy, gc, k):
        if kind == "X":
            return xbuf.at[row_of(dx, dy, gc), pl.ds(*k), :]
        gy = yl if dy == 0 else 1 - yl
        return ybuf.at[2 * gy + gc, pl.ds(k * PK, PK), :]

    def copy_of(src, dst, ssem, rsem, to):
        return pltpu.make_async_remote_copy(
            src_ref=src, dst_ref=dst, send_sem=ssem, recv_sem=rsem,
            device_id=dev[to], device_id_type=MESH,
        )

    def send(link, kind, dx, dy, k):
        i = LINK_ID[(link, kind, dx, dy, k)]
        sign = 1 if link == "+" else -1
        if kind == "P":
            src = pbuf.at[SLOT[dx], k]
            dst = pbuf.at[SLOT[-sign] if dx == 0 else SLOT[2], k]
        elif kind == "M":
            part = pl.ds(0 if sign > 0 else 2, 2)
            if dx == sign:
                src, dst = mout.at[SLOT[sign] - 1], minto.at[SLOT[-sign] - 1]
            elif k == 0:
                src, dst = mout.at[SLOT[2] - 1, part], mrel.at[0 if sign > 0 else 1]
            else:
                src, dst = mrel.at[0 if sign > 0 else 1], minto.at[SLOT[2] - 1, part]
        else:
            src = dst = piece(kind, dx, dy, core, k)
        copy_of(src, dst, ls, lr.at[i], link).start()

    def core_send(kind, dx, dy, k):
        i = CORE_ID[(kind, dx, dy, k)]
        ref = piece(kind, dx, dy, core, k)
        copy_of(ref, ref, cs, cr.at[i], "c").start()

    def core_recv(kind, dx, dy, k):
        i = CORE_ID[(kind, dx, dy, k)]
        ref = piece(kind, dx, dy, 1 - core, k)
        copy = copy_of(ref, ref, cs, cr.at[i], "c")
        copy.wait_recv()

    def await_link(link, sender, ref):
        copy = copy_of(ref, ref, ls, lr.at[LINK_ID[(link,) + sender]], link)
        copy.wait_recv()

    def recv(link, kind, dx, dy, k):
        if link == "y":
            sender = (kind, dx, 1 - dy, k)
        elif link == "+":
            sender = (kind, (dx + 2) % 4 - 1, dy, k)
        else:
            sender = (kind, dx % 4 - 1, dy, k)
        await_link(link, sender, piece(kind, dx, dy, core, k))
        core_send(kind, dx, dy, k)

    def recv_p(dx, q):
        if dx == 2:
            sign = 1 if q < 2 else -1
            sender = ("P", -sign, 0, q)
        else:
            sign = -dx
            sender = ("P", 0, 0, q)
        await_link("+" if sign > 0 else "-", sender, pbuf.at[SLOT[dx], q])

    me = tile

    def raw(n, k):
        return vbuf.at[3, n, pl.ds(k // 2 * B, B), pl.ds(k % 2 * PK, PK)]

    def columns(ref, k):
        return ref.at[:, pl.ds(k * PK, PK)]

    y_loads, p_loads, q_loads = [], [], []
    for k in range(CH):
        y_loads.append(pltpu.make_async_copy(columns(yin, k), raw(0, k), in_sem.at[k]))
        p_loads.append(pltpu.make_async_copy(columns(pin, k), pbuf.at[0, k], in_sem.at[CH + k]))
        q_loads.append(pltpu.make_async_copy(columns(qin, k), raw(1, k), in_sem.at[2 * CH + k]))
    x_load = pltpu.make_async_copy(xin, xbuf.at[me], in_sem.at[3 * CH])
    for copy in y_loads + p_loads + [x_load] + q_loads:
        copy.start()

    barrier = pltpu.get_barrier_semaphore()
    for name in ("y", "+", "-", "c", "z+", "z-"):
        pl.semaphore_signal(barrier, inc=1, device_id=dev[name], device_id_type=MESH)

    col = lax.broadcasted_iota(jnp.int32, (8, K), 1)

    def keep(ranks):
        limit = jnp.zeros((8, K), jnp.int32)
        for k in range(KP):
            limit = jnp.where(col // R == k, ranks[k], limit)
        return (col % R < limit).astype(F32)[:1]

    lkeep = keep(lrank)

    def turn_y(k):
        y_loads[k].wait()
        part = raw(0, k)[...].astype(F32) * lkeep[:, k * PK : (k + 1) * PK]
        ybuf[2 * yl + core, k * PK : (k + 1) * PK, :] = part.T.astype(BF)

    def send_y(k):
        send("y", "Y", 0, 0, k)
        core_send("Y", 0, 0, k)

    turn_y(0)
    pl.semaphore_wait(barrier, 6)
    send_y(0)
    ukeep = keep(urank)

    def mask_p(k):
        p_loads[k].wait()
        pbuf[0, k] = (pbuf[0, k].astype(F32) * ukeep[:, k * PK : (k + 1) * PK]).astype(BF)

    def send_p(k):
        send("+", "P", 0, 0, k)
        send("-", "P", 0, 0, k)

    mask_p(0)
    turn_y(1)
    send_p(0)
    for k in range(1, CH):
        mask_p(k)
        if k + 1 < CH:
            turn_y(k + 1)
        send_y(k)
        send_p(k)
    x_load.wait()
    for h in HALVES:
        send("y", "X", 0, 0, h)
    core_send("X", 0, 0, FULL)
    for k in range(CH):
        q_loads[k].wait()
        qtbuf[k * PK : (k + 1) * PK, :] = raw(1, k)[...].astype(F32).T.astype(BF)

    def same_panel():
        a = lax.broadcasted_iota(jnp.int32, (PK, PK), 0) // R
        return a == lax.broadcasted_iota(jnp.int32, (PK, PK), 1) // R

    def middle(r, slot, q):
        rows = slice(q * PK, (q + 1) * PK)
        m = jnp.dot(ybuf[r, rows, :], pbuf[slot, q], preferred_element_type=F32)
        return jnp.where(same_panel(), m, 0.0)

    def put_v(slot, rs, q, middles):
        rows = slice(q * PK, (q + 1) * PK)
        for r, m in zip(rs, middles):
            v = jnp.dot(m, qtbuf[rows, :], preferred_element_type=F32)
            vbuf[slot, r, rows, :] = v.astype(BF)

    def own_v(dy, k, classes=(0, 1)):
        gy = yl if dy == 0 else 1 - yl
        rs = [2 * gy + (core if c == 0 else 1 - core) for c in classes]
        put_v(0, rs, k, [middle(r, 0, k).astype(BF) for r in rs])

    def make_m(dx, q):
        for r in range(4):
            m = middle(r, SLOT[dx], q)
            m = m[:, : PK // 2] + m[:, PK // 2 :]
            for t in range(2):
                part = [m[t * 128 + i * R : t * 128 + (i + 1) * R] for i in range(4)]
                mout[SLOT[dx] - 1, q, r, t * R : (t + 1) * R, :] = (part[0] + part[1] + part[2] + part[3]).astype(BF)

    def far_v(dx, q):
        middles = []
        for r in range(4):
            m = minto[SLOT[dx] - 1, q, r].astype(F32)
            m = jnp.concatenate([m[:R]] * 4 + [m[R:]] * 4, axis=0)
            m = jnp.concatenate([m, m], axis=1)
            middles.append(jnp.where(same_panel(), m, 0.0).astype(BF))
        put_v(SLOT[dx], range(4), q, middles)

    col_half = [halves[4 * yh + c, tile] for c in range(4)]
    col_shift = [shifts[yh, tile + 16 * col_half[c]] for c in range(4)]
    half = halves[front, tile]
    shift = shifts[yh, tile + 16 * half]

    def sum_of(n):
        dx, (row, _) = Z_STEPS[n]
        return SUMS.index((dx, row // PR))

    def z_copy(n, what, src, dst, to):
        rsem = zr.at[n] if what < 2 else zlast.at[sum_of(n)]
        return copy_of(src, dst, zs, rsem, to)

    def z_send(n, what):
        dx, (row, rows) = Z_STEPS[n]
        g = (x + dx + 4) % 4
        hr, at = rows // 2, Z_AT[n]
        passing = [relay.at[i, pl.ds(at // 2, hr), :] for i in range(2)]
        src, dst, to = [
            (sbuf.at[1, pl.ds(at, hr), :], passing[0], "z+"),
            (sbuf.at[1, pl.ds(at + hr, hr), :], passing[1], "z-"),
            (sbuf.at[0, pl.ds(at, rows), :], out.at[z, g, pl.ds(row, rows), :], "z+"),
            (sbuf.at[2, pl.ds(at, rows), :], out.at[z, g, pl.ds(row, rows), :], "z-"),
            (passing[0], out.at[(z + 3) % 4, g, pl.ds(row, hr), :], "z+"),
            (passing[1], out.at[(z + 1) % 4, g, pl.ds(row + hr, hr), :], "z-"),
        ][what]
        z_copy(n, what, src, dst, to).start()

    def hand_on(n):
        _, (_, rows) = Z_STEPS[n]
        both = relay.at[:, pl.ds(Z_AT[n] // 2, rows // 2), :]
        copy = z_copy(n, 0, both, both, "z+")
        copy.wait_recv()
        for what in (4, 5):
            z_send(n, what)

    handed = []

    def relay_upto(n):
        while len(handed) <= n:
            hand_on(len(handed))
            handed.append(n)

    def sum_step(n):
        dx, k = SUMS[n]
        g = (x + dx + 4) % 4
        theirs = out.at[pl.ds(0, 3), g, pl.ds(k * PR, PR), :]
        copy = copy_of(theirs, theirs, zs, zlast.at[n], "z+")
        copy.wait_recv()
        place = []
        for c in range(4):
            row = 4 * g + (z - col_shift[c] + 4) % 4
            place.append(2 * col_half[c] + halves[4 * yh + c, row])
        depth = 16

        def body(i, carry):
            rows = pl.ds(pl.multiple_of(k * PR + i * depth, depth), depth)
            tiles = [out[c, g, rows, :].astype(jnp.float32) for c in range(4)]
            for s in range(4):
                total = jnp.zeros((depth, B), jnp.float32)
                for c in range(4):
                    total = total + jnp.where(place[c] == s, tiles[c], 0.0)
                out[s, g, rows, :] = total.astype(BF)
            return carry

        lax.fori_loop(0, PR // depth, body, 0)

    pending = []

    def later(work, *args):
        pending.append(functools.partial(work, *args))

    def run_some(count):
        for _ in range(min(count, len(pending))):
            pending.pop(0)()

    def z_step(n):
        dx, (row, rows) = Z_STEPS[n]
        g = (x + dx + 4) % 4
        at = Z_AT[n]

        def tiles_of(gc):
            for gy in range(2):
                r = 2 * gy + gc
                acc = jnp.dot(
                    xbuf[g * 4 + r, pl.ds(row, rows), :], vbuf[SLOT[dx], r], preferred_element_type=F32
                )
                stage[r, :rows] = acc.astype(BF)

        tiles_of(core)
        run_some(1)
        if dx != 0:
            core_recv("X", dx, 0, (row, rows))
        elif n == 0:
            core_recv("X", 0, 0, FULL)
        core_recv("X", dx, 1, (row, rows))
        tiles_of(1 - core)
        for rel in (2, 1, 3):
            sbuf[rel - 1, at : at + rows, :] = stage[(z + rel - shift + 4) % 4, :rows]
        for what in (0, 1, 2, 3):
            z_send(n, what)
        out[z, g, row : row + rows, :] = stage[(z - shift + 4) % 4, :rows]

    def pass_on(link, dx, k):
        recv(link, "X", dx, 0, piece_rows(k))
        send("y", "X", dx, 0, piece_rows(k))

    both = (("-", 1), ("+", -1))

    for k in range(CH):
        own_v(0, k, (0,))
    for k in range(CH):
        core_recv("Y", 0, 0, k)
        own_v(0, k, (1,))
    for k in range(CH):
        recv("y", "Y", 0, 1, k)
        if k == 3:
            own_v(1, k, (0,))
        for dx in (1, -1):
            recv_p(dx, k)
        if k == 3:
            for link, _ in both:
                send(link, "X", 0, 0, piece_rows(0))
        core_recv("Y", 0, 1, k)
        own_v(1, k, (0, 1) if k < 3 else (1,))
        make_m(1, k)
        make_m(-1, k)
    send("+", "M", 1, 0, 0)
    send("-", "M", -1, 0, 0)
    for h in range(2 * CH):
        recv("y", "X", 0, 1, HALVES[h])
        if h == 1:
            for link, dx in both:
                send(link, "X", 0, 1, piece_rows(0))
                send(link, "X", 0, 0, piece_rows(1))
                for q, k in ((0, 2), (1, 3)) if link == "+" else ((2, 2), (3, 3)):
                    send(link, "P", dx, 0, q)
                    send(link, "X", 0, 0, piece_rows(k))
        z_step(h)
        relay_upto(h - 1)
        if h == 2:
            for link, dx in both:
                recv(link, "X", dx, 0, piece_rows(0))
        if h == 4:
            await_link("-", ("M", -1, 0, 0), minto.at[SLOT[1] - 1])
            await_link("+", ("M", 1, 0, 0), minto.at[SLOT[-1] - 1])
            for q in range(CH):
                later(far_v, 1, q)
            for q in range(CH):
                later(far_v, -1, q)
        if h == 5:
            for link, dx in both:
                recv(link, "X", dx, 1, piece_rows(0))
        if h == 7:
            for link, dx in both:
                pass_on(link, dx, 1)
        if h > 4:
            run_some(1)
    for n in range(8, 20):
        dx, (row, _) = Z_STEPS[n]
        if n == 9:
            run_some(len(pending))
        if 10 <= n < 16:
            recv("y", "X", dx, 1, (row, PR))
        z_step(n)
        relay_upto(n - 1 if n < 17 else n - 2)
        if n in (8, 10):
            for q in (0, 2) if n == 8 else (1, 3):
                recv_p(2, q)
                make_m(2, q)
        if n == 10:
            send("+", "M", 2, 0, 0)
            send("-", "M", 2, 0, 0)
        if n in (9, 11):
            for link, e in both:
                pass_on(link, e, 2 if n == 9 else 3)
        if n == 10:
            for k in (0, 1):
                send("+", "X", -1, 0, piece_rows(k))
            send("-", "X", 1, 0, piece_rows(2))
        if n == 11:
            send("-", "X", 1, 0, piece_rows(3))
        if n == 12:
            for link, i in (("+", 0), ("-", 1)):
                await_link(link, ("M", 2, 0, 0), mrel.at[i])
                send(link, "M", 2, 0, 1)
            send("+", "X", -1, 1, piece_rows(0))
            send("+", "X", -1, 1, piece_rows(1))
            send("-", "X", 1, 1, piece_rows(2))
        if n == 13:
            recv("+", "X", 2, 0, piece_rows(0))
            recv("-", "X", 2, 0, piece_rows(2))
        if n == 14:
            send("-", "X", 1, 1, piece_rows(3))
            recv("+", "X", 2, 0, piece_rows(1))
            recv("-", "X", 2, 0, piece_rows(3))
        if n == 15:
            for link, i in (("+", 0), ("-", 2)):
                await_link(link, ("M", 2, 0, 1), minto.at[SLOT[2] - 1, pl.ds(i, 2)])
            for q in range(CH):
                far_v(2, q)
            recv("+", "X", 2, 1, piece_rows(0))
            recv("-", "X", 2, 1, piece_rows(2))
        if n == 17:
            recv("+", "X", 2, 1, piece_rows(1))
            recv("-", "X", 2, 1, piece_rows(3))
        if 10 <= n < 18:
            later(sum_step, n - 10)
    while pending:
        run_some(1)
    for n in (18, 19):
        relay_upto(n)
    for n in range(8, 16):
        sum_step(n)
    twelve, ten = xbuf.at[pl.ds(0, 12)], xbuf.at[pl.ds(0, 10)]
    copy_of(twelve, twelve, ls, lr.at[0], "y").wait_send()
    copy_of(ten, ten, cs, cr.at[0], "c").wait_send()
    copy_of(out, out, zs, zlast.at[0], "z+").wait_send()


def main_call(xin, yin, pin, qin, lrank, urank, halves, shifts):
    hbm = pl.BlockSpec(memory_space=pl.ANY)
    smem = pl.BlockSpec(memory_space=pltpu.SMEM)
    return pl.pallas_call(
        main_kernel,
        out_shape=pltpu.VMEM((4, 4, B, B), BF),
        in_specs=[smem] * 4 + [hbm] * 4,
        out_specs=pl.BlockSpec(memory_space=pltpu.VMEM),
        scratch_shapes=[
            pltpu.VMEM((16, B, K), BF),
            pltpu.VMEM((4, K, B), BF),
            pltpu.VMEM((4, 4, K, B), BF),
            pltpu.VMEM((4, CH, B, PK), BF),
            pltpu.VMEM((3, CH, 4, 2 * R, 128), BF),
            pltpu.VMEM((3, CH, 4, 2 * R, 128), BF),
            pltpu.VMEM((2, 2, 4, 2 * R, 128), BF),
            pltpu.VMEM((K, B), BF),
            pltpu.VMEM((4, PR, B), BF),
            pltpu.VMEM((3, 4 * B, B), BF),
            pltpu.VMEM((2, 2 * B, B), BF),
            pltpu.SemaphoreType.DMA((3 * CH + 1,)),
            pltpu.SemaphoreType.DMA,
            pltpu.SemaphoreType.DMA((len(LINK_OPS),)),
            pltpu.SemaphoreType.DMA,
            pltpu.SemaphoreType.DMA((len(CORE_OPS),)),
            pltpu.SemaphoreType.DMA,
            pltpu.SemaphoreType.DMA((len(Z_STEPS),)),
            pltpu.SemaphoreType.DMA((len(SUMS),)),
        ],
        compiler_params=pltpu.CompilerParams(
            collective_id=0, has_side_effects=True, vmem_limit_bytes=58_000_000
        ),
        name="gather_update_exchange",
    )(lrank, urank, halves, shifts, xin, yin, pin, qin)


def per_device(lower_basis, lower_coeff, upper_basis, upper_coeff, lower_rank, upper_rank, child_half, owner_shift):
    blocks = main_call(
        lower_basis[0, 0], lower_coeff[0, 0], upper_basis[0, 0], upper_coeff[0, 0],
        lower_rank[0, 0], upper_rank[0, 0], child_half, owner_shift,
    )
    return blocks.reshape(1, 1, 16 * B, B)


def solution(mesh):
    whole = P("front", "tile", None, None)
    ranks = P("front", "tile", None)
    return jax.shard_map(
        per_device,
        mesh=mesh,
        in_specs=(whole, whole, whole, whole, ranks, ranks, P(), P()),
        out_specs=whole,
        check_vma=False,
    )
```

```python
import functools

import jax
import jax.numpy as jnp
from jax import lax
from jax.experimental import pallas as pl
from jax.experimental.pallas import tpu as pltpu
from jax.sharding import PartitionSpec as P

MESH = pl.DeviceIdType.MESH
B = 512
R = 32
KP = 32
K = 1024
CH = 4
PR = B // CH
PK = K // CH
BF = jnp.bfloat16
F32 = jnp.float32


def piece_rows(k):
    return (k * PR, PR)


FULL = (0, B)
HALVES = [(i * PR // 2, PR // 2) for i in range(2 * CH)]

Y_OPS = (
    [("Y", 0, 0, k) for k in range(CH)]
    + [("X", 0, 0, h) for h in HALVES]
    + [("X", d, 0, piece_rows(k)) for k in range(1, CH) for d in (1, -1)]
)


def x_ops(sign):
    a, b = (0, 1) if sign > 0 else (2, 3)
    return (
        [("P", 0, 0, q) for q in range(CH)]
        + [("P", -sign, 0, a), ("P", -sign, 0, b)]
        + [("X", 0, 0, piece_rows(k)) for k in range(CH)]
        + [("X", 0, 1, piece_rows(0))]
        + [("X", -sign, dy, piece_rows(k)) for dy in (0, 1) for k in (a, b)]
        + [("M", sign, 0, 0), ("M", 2, 0, 0), ("M", 2, 0, 1)]
    )


LINK_OPS = [("y",) + op for op in Y_OPS] + [("+",) + op for op in x_ops(1)] + [("-",) + op for op in x_ops(-1)]
LINK_ID = {op: i for i, op in enumerate(LINK_OPS)}
CORE_OPS = (
    [("Y", 0, dy, k) for dy in (0, 1) for k in range(CH)]
    + [("X", 0, 0, FULL)]
    + [("X", 0, 1, h) for h in HALVES]
    + [("X", dx, dy, piece_rows(k)) for dx in (1, -1, 2) for dy in (0, 1) for k in range(CH)]
)
CORE_ID = {op: i for i, op in enumerate(CORE_OPS)}
Z_STEPS = (
    [(0, h) for h in HALVES]
    + [(d, piece_rows(k)) for k in range(CH) for d in (1, -1)]
    + [(2, piece_rows(k)) for k in (0, 2, 1, 3)]
)
SUMS = [(0, k) for k in range(CH)] + [(dx, row // PR) for dx, (row, _) in Z_STEPS[2 * CH :]]
Z_AT = [sum(rows for _, (_, rows) in Z_STEPS[:n]) for n in range(len(Z_STEPS))]
SLOT = {0: 0, 1: 1, -1: 2, 2: 3}


def main_kernel(
    lrank, urank, halves, shifts, xin, yin, pin, qin, out,
    xbuf, ybuf, vbuf, pbuf, mout, minto, mrel, qtbuf, stage, sbuf, relay,
    in_sem, ls, lr, cs, cr, zs, zr, zlast,
):
    front, tile = lax.axis_index("front"), lax.axis_index("tile")
    yh, z = front // 4, front % 4
    x, yl, core = tile // 4, (tile // 2) % 2, tile % 2

    def tile_at(gx, gy, gc):
        return (gx * 2 + gy) * 2 + gc

    dev = {
        "y": (front, tile_at(x, 1 - yl, core)),
        "+": (front, tile_at((x + 1) % 4, yl, core)),
        "-": (front, tile_at((x + 3) % 4, yl, core)),
        "c": (front, tile_at(x, yl, 1 - core)),
        "z+": (yh * 4 + (z + 1) % 4, tile),
        "z-": (yh * 4 + (z + 3) % 4, tile),
    }

    def row_of(dx, dy, gc):
        gy = yl if dy == 0 else 1 - yl
        return tile_at((x + dx + 4) % 4, gy, gc)

    def piece(kind, dx, dy, gc, k):
        if kind == "X":
            return xbuf.at[row_of(dx, dy, gc), pl.ds(*k), :]
        gy = yl if dy == 0 else 1 - yl
        return ybuf.at[2 * gy + gc, pl.ds(k * PK, PK), :]

    def copy_of(src, dst, ssem, rsem, to):
        return pltpu.make_async_remote_copy(
            src_ref=src, dst_ref=dst, send_sem=ssem, recv_sem=rsem,
            device_id=dev[to], device_id_type=MESH,
        )

    def send(link, kind, dx, dy, k):
        i = LINK_ID[(link, kind, dx, dy, k)]
        sign = 1 if link == "+" else -1
        if kind == "P":
            src = pbuf.at[SLOT[dx], k]
            dst = pbuf.at[SLOT[-sign] if dx == 0 else SLOT[2], k]
        elif kind == "M":
            part = pl.ds(0 if sign > 0 else 2, 2)
            if dx == sign:
                src, dst = mout.at[SLOT[sign] - 1], minto.at[SLOT[-sign] - 1]
            elif k == 0:
                src, dst = mout.at[SLOT[2] - 1, part], mrel.at[0 if sign > 0 else 1]
            else:
                src, dst = mrel.at[0 if sign > 0 else 1], minto.at[SLOT[2] - 1, part]
        else:
            src = dst = piece(kind, dx, dy, core, k)
        copy_of(src, dst, ls, lr.at[i], link).start()

    def core_send(kind, dx, dy, k):
        i = CORE_ID[(kind, dx, dy, k)]
        ref = piece(kind, dx, dy, core, k)
        copy_of(ref, ref, cs, cr.at[i], "c").start()

    def core_recv(kind, dx, dy, k):
        i = CORE_ID[(kind, dx, dy, k)]
        ref = piece(kind, dx, dy, 1 - core, k)
        copy = copy_of(ref, ref, cs, cr.at[i], "c")
        copy.wait_recv()

    def await_link(link, sender, ref):
        copy = copy_of(ref, ref, ls, lr.at[LINK_ID[(link,) + sender]], link)
        copy.wait_recv()

    def recv(link, kind, dx, dy, k):
        if link == "y":
            sender = (kind, dx, 1 - dy, k)
        elif link == "+":
            sender = (kind, (dx + 2) % 4 - 1, dy, k)
        else:
            sender = (kind, dx % 4 - 1, dy, k)
        await_link(link, sender, piece(kind, dx, dy, core, k))
        core_send(kind, dx, dy, k)

    def recv_p(dx, q):
        if dx == 2:
            sign = 1 if q < 2 else -1
            sender = ("P", -sign, 0, q)
        else:
            sign = -dx
            sender = ("P", 0, 0, q)
        await_link("+" if sign > 0 else "-", sender, pbuf.at[SLOT[dx], q])

    me = tile

    def raw(n, k):
        return vbuf.at[3, n, pl.ds(k // 2 * B, B), pl.ds(k % 2 * PK, PK)]

    def columns(ref, k):
        return ref.at[:, pl.ds(k * PK, PK)]

    y_loads, p_loads, q_loads = [], [], []
    for k in range(CH):
        y_loads.append(pltpu.make_async_copy(columns(yin, k), raw(0, k), in_sem.at[k]))
        p_loads.append(pltpu.make_async_copy(columns(pin, k), pbuf.at[0, k], in_sem.at[CH + k]))
        q_loads.append(pltpu.make_async_copy(columns(qin, k), raw(1, k), in_sem.at[2 * CH + k]))
    x_load = pltpu.make_async_copy(xin, xbuf.at[me], in_sem.at[3 * CH])
    for copy in y_loads + p_loads + [x_load] + q_loads:
        copy.start()

    barrier = pltpu.get_barrier_semaphore()
    for name in ("y", "+", "-", "c", "z+", "z-"):
        pl.semaphore_signal(barrier, inc=1, device_id=dev[name], device_id_type=MESH)

    col = lax.broadcasted_iota(jnp.int32, (8, K), 1)

    def keep(ranks):
        limit = jnp.zeros((8, K), jnp.int32)
        for k in range(KP):
            limit = jnp.where(col // R == k, ranks[k], limit)
        return (col % R < limit).astype(F32)[:1]

    lkeep = keep(lrank)

    def turn_y(k):
        y_loads[k].wait()
        part = raw(0, k)[...].astype(F32) * lkeep[:, k * PK : (k + 1) * PK]
        ybuf[2 * yl + core, k * PK : (k + 1) * PK, :] = part.T.astype(BF)

    def send_y(k):
        send("y", "Y", 0, 0, k)
        core_send("Y", 0, 0, k)

    turn_y(0)
    pl.semaphore_wait(barrier, 6)
    send_y(0)
    ukeep = keep(urank)

    def mask_p(k):
        p_loads[k].wait()
        pbuf[0, k] = (pbuf[0, k].astype(F32) * ukeep[:, k * PK : (k + 1) * PK]).astype(BF)

    def send_p(k):
        send("+", "P", 0, 0, k)
        send("-", "P", 0, 0, k)

    mask_p(0)
    turn_y(1)
    send_p(0)
    for k in range(1, CH):
        mask_p(k)
        if k + 1 < CH:
            turn_y(k + 1)
        send_y(k)
        send_p(k)
    x_load.wait()
    for h in HALVES:
        send("y", "X", 0, 0, h)
    core_send("X", 0, 0, FULL)
    for k in range(CH):
        q_loads[k].wait()
        qtbuf[k * PK : (k + 1) * PK, :] = raw(1, k)[...].astype(F32).T.astype(BF)

    def same_panel():
        a = lax.broadcasted_iota(jnp.int32, (PK, PK), 0) // R
        return a == lax.broadcasted_iota(jnp.int32, (PK, PK), 1) // R

    def middle(r, slot, q):
        rows = slice(q * PK, (q + 1) * PK)
        m = jnp.dot(ybuf[r, rows, :], pbuf[slot, q], preferred_element_type=F32)
        return jnp.where(same_panel(), m, 0.0)

    def put_v(slot, rs, q, middles):
        rows = slice(q * PK, (q + 1) * PK)
        for r, m in zip(rs, middles):
            v = jnp.dot(m, qtbuf[rows, :], preferred_element_type=F32)
            vbuf[slot, r, rows, :] = v.astype(BF)

    def own_v(dy, k, classes=(0, 1)):
        gy = yl if dy == 0 else 1 - yl
        rs = [2 * gy + (core if c == 0 else 1 - core) for c in classes]
        put_v(0, rs, k, [middle(r, 0, k).astype(BF) for r in rs])

    def make_m(dx, q):
        for r in range(4):
            m = middle(r, SLOT[dx], q)
            m = m[:, : PK // 2] + m[:, PK // 2 :]
            for t in range(2):
                part = [m[t * 128 + i * R : t * 128 + (i + 1) * R] for i in range(4)]
                mout[SLOT[dx] - 1, q, r, t * R : (t + 1) * R, :] = (part[0] + part[1] + part[2] + part[3]).astype(BF)

    def far_v(dx, q):
        middles = []
        for r in range(4):
            m = minto[SLOT[dx] - 1, q, r].astype(F32)
            m = jnp.concatenate([m[:R]] * 4 + [m[R:]] * 4, axis=0)
            m = jnp.concatenate([m, m], axis=1)
            middles.append(jnp.where(same_panel(), m, 0.0).astype(BF))
        put_v(SLOT[dx], range(4), q, middles)

    col_half = [halves[4 * yh + c, tile] for c in range(4)]
    col_shift = [shifts[yh, tile + 16 * col_half[c]] for c in range(4)]
    half = halves[front, tile]
    shift = shifts[yh, tile + 16 * half]

    def sum_of(n):
        dx, (row, _) = Z_STEPS[n]
        return SUMS.index((dx, row // PR))

    def z_copy(n, what, src, dst, to):
        rsem = zr.at[n] if what < 2 else zlast.at[sum_of(n)]
        return copy_of(src, dst, zs, rsem, to)

    def z_send(n, what):
        dx, (row, rows) = Z_STEPS[n]
        g = (x + dx + 4) % 4
        hr, at = rows // 2, Z_AT[n]
        passing = [relay.at[i, pl.ds(at // 2, hr), :] for i in range(2)]
        src, dst, to = [
            (sbuf.at[1, pl.ds(at, hr), :], passing[0], "z+"),
            (sbuf.at[1, pl.ds(at + hr, hr), :], passing[1], "z-"),
            (sbuf.at[0, pl.ds(at, rows), :], out.at[z, g, pl.ds(row, rows), :], "z+"),
            (sbuf.at[2, pl.ds(at, rows), :], out.at[z, g, pl.ds(row, rows), :], "z-"),
            (passing[0], out.at[(z + 3) % 4, g, pl.ds(row, hr), :], "z+"),
            (passing[1], out.at[(z + 1) % 4, g, pl.ds(row + hr, hr), :], "z-"),
        ][what]
        z_copy(n, what, src, dst, to).start()

    def hand_on(n):
        _, (_, rows) = Z_STEPS[n]
        both = relay.at[:, pl.ds(Z_AT[n] // 2, rows // 2), :]
        copy = z_copy(n, 0, both, both, "z+")
        copy.wait_recv()
        for what in (4, 5):
            z_send(n, what)

    handed = []

    def relay_upto(n):
        while len(handed) <= n:
            hand_on(len(handed))
            handed.append(n)

    def sum_step(n):
        dx, k = SUMS[n]
        g = (x + dx + 4) % 4
        theirs = out.at[pl.ds(0, 3), g, pl.ds(k * PR, PR), :]
        copy = copy_of(theirs, theirs, zs, zlast.at[n], "z+")
        copy.wait_recv()
        place = []
        for c in range(4):
            row = 4 * g + (z - col_shift[c] + 4) % 4
            place.append(2 * col_half[c] + halves[4 * yh + c, row])
        depth = 16

        def body(i, carry):
            rows = pl.ds(pl.multiple_of(k * PR + i * depth, depth), depth)
            tiles = [out[c, g, rows, :].astype(jnp.float32) for c in range(4)]
            for s in range(4):
                total = jnp.zeros((depth, B), jnp.float32)
                for c in range(4):
                    total = total + jnp.where(place[c] == s, tiles[c], 0.0)
                out[s, g, rows, :] = total.astype(BF)
            return carry

        lax.fori_loop(0, PR // depth, body, 0)

    pending = []

    def later(work, *args):
        pending.append(functools.partial(work, *args))

    def run_some(count):
        for _ in range(min(count, len(pending))):
            pending.pop(0)()

    def z_step(n):
        dx, (row, rows) = Z_STEPS[n]
        g = (x + dx + 4) % 4
        at = Z_AT[n]

        def tiles_of(gc):
            for gy in range(2):
                r = 2 * gy + gc
                acc = jnp.dot(
                    xbuf[g * 4 + r, pl.ds(row, rows), :], vbuf[SLOT[dx], r], preferred_element_type=F32
                )
                stage[r, :rows] = acc.astype(BF)

        tiles_of(core)
        if n != 8:
            run_some(1)
        if dx != 0:
            core_recv("X", dx, 0, (row, rows))
        elif n == 0:
            core_recv("X", 0, 0, FULL)
        core_recv("X", dx, 1, (row, rows))
        tiles_of(1 - core)
        for rel in (2, 1, 3):
            sbuf[rel - 1, at : at + rows, :] = stage[(z + rel - shift + 4) % 4, :rows]
        for what in (0, 1, 2, 3):
            z_send(n, what)
        out[z, g, row : row + rows, :] = stage[(z - shift + 4) % 4, :rows]

    def pass_on(link, dx, k):
        recv(link, "X", dx, 0, piece_rows(k))
        send("y", "X", dx, 0, piece_rows(k))

    both = (("-", 1), ("+", -1))

    for k in range(CH):
        own_v(0, k, (0,))
    for k in range(CH):
        core_recv("Y", 0, 0, k)
        own_v(0, k, (1,))
    for k in range(CH):
        recv("y", "Y", 0, 1, k)
        if k == 3:
            own_v(1, k, (0,))
        for dx in (1, -1):
            recv_p(dx, k)
        if k == 3:
            for link, _ in both:
                send(link, "X", 0, 0, piece_rows(0))
        core_recv("Y", 0, 1, k)
        own_v(1, k, (0, 1) if k < 3 else (1,))
        make_m(1, k)
        make_m(-1, k)
    send("+", "M", 1, 0, 0)
    send("-", "M", -1, 0, 0)
    for h in range(2 * CH):
        recv("y", "X", 0, 1, HALVES[h])
        if h == 1:
            for link, dx in both:
                send(link, "X", 0, 1, piece_rows(0))
                send(link, "X", 0, 0, piece_rows(1))
                for q, k in ((0, 2), (1, 3)) if link == "+" else ((2, 2), (3, 3)):
                    send(link, "P", dx, 0, q)
                    send(link, "X", 0, 0, piece_rows(k))
        z_step(h)
        relay_upto(h - 1)
        if h == 2:
            for link, dx in both:
                recv(link, "X", dx, 0, piece_rows(0))
        if h == 4:
            await_link("-", ("M", -1, 0, 0), minto.at[SLOT[1] - 1])
            await_link("+", ("M", 1, 0, 0), minto.at[SLOT[-1] - 1])
            for q in range(CH):
                later(far_v, 1, q)
            for q in range(CH):
                later(far_v, -1, q)
        if h == 5:
            for link, dx in both:
                recv(link, "X", dx, 1, piece_rows(0))
        if h == 7:
            for link, dx in both:
                pass_on(link, dx, 1)
        if 4 < h < 7:
            run_some(1)

    def second_hop():
        for link, e in both:
            pass_on(link, e, 2)

    for n in range(8, 20):
        if n == 10:
            pending.insert(0, second_hop)
        z_step(n)
        if 10 <= n + 1 < 16:
            ahead = Z_STEPS[n + 1]
            recv("y", "X", ahead[0], 1, ahead[1])
        relay_upto(n - 1 if n < 17 else n - 2)
        if n == 8:
            run_some(len(pending))
        if n in (8, 10):
            for q in (0, 2) if n == 8 else (1, 3):
                recv_p(2, q)
                make_m(2, q)
        if n == 10:
            send("+", "M", 2, 0, 0)
            send("-", "M", 2, 0, 0)
        if n == 11:
            for link, e in both:
                pass_on(link, e, 3)
        if n == 10:
            for k in (0, 1):
                send("+", "X", -1, 0, piece_rows(k))
            send("-", "X", 1, 0, piece_rows(2))
        if n == 11:
            send("-", "X", 1, 0, piece_rows(3))
        if n == 12:
            for link, i in (("+", 0), ("-", 1)):
                await_link(link, ("M", 2, 0, 0), mrel.at[i])
                send(link, "M", 2, 0, 1)
            send("+", "X", -1, 1, piece_rows(0))
            send("+", "X", -1, 1, piece_rows(1))
            send("-", "X", 1, 1, piece_rows(2))
        if n == 13:
            recv("+", "X", 2, 0, piece_rows(0))
            recv("-", "X", 2, 0, piece_rows(2))
        if n == 14:
            send("-", "X", 1, 1, piece_rows(3))
            recv("+", "X", 2, 0, piece_rows(1))
            recv("-", "X", 2, 0, piece_rows(3))
        if n == 15:
            for link, i in (("+", 0), ("-", 2)):
                await_link(link, ("M", 2, 0, 1), minto.at[SLOT[2] - 1, pl.ds(i, 2)])
            for q in range(CH):
                far_v(2, q)
            recv("+", "X", 2, 1, piece_rows(0))
            recv("-", "X", 2, 1, piece_rows(2))
        if n == 17:
            recv("+", "X", 2, 1, piece_rows(1))
            recv("-", "X", 2, 1, piece_rows(3))
        if 10 <= n < 18:
            later(sum_step, n - 10)
    while pending:
        run_some(1)
    for n in (18, 19):
        relay_upto(n)
    for n in range(8, 16):
        sum_step(n)
    twelve, ten = xbuf.at[pl.ds(0, 12)], xbuf.at[pl.ds(0, 10)]
    copy_of(twelve, twelve, ls, lr.at[0], "y").wait_send()
    copy_of(ten, ten, cs, cr.at[0], "c").wait_send()
    copy_of(out, out, zs, zlast.at[0], "z+").wait_send()


def main_call(xin, yin, pin, qin, lrank, urank, halves, shifts):
    hbm = pl.BlockSpec(memory_space=pl.ANY)
    smem = pl.BlockSpec(memory_space=pltpu.SMEM)
    return pl.pallas_call(
        main_kernel,
        out_shape=pltpu.VMEM((4, 4, B, B), BF),
        in_specs=[smem] * 4 + [hbm] * 4,
        out_specs=pl.BlockSpec(memory_space=pltpu.VMEM),
        scratch_shapes=[
            pltpu.VMEM((16, B, K), BF),
            pltpu.VMEM((4, K, B), BF),
            pltpu.VMEM((4, 4, K, B), BF),
            pltpu.VMEM((4, CH, B, PK), BF),
            pltpu.VMEM((3, CH, 4, 2 * R, 128), BF),
            pltpu.VMEM((3, CH, 4, 2 * R, 128), BF),
            pltpu.VMEM((2, 2, 4, 2 * R, 128), BF),
            pltpu.VMEM((K, B), BF),
            pltpu.VMEM((4, PR, B), BF),
            pltpu.VMEM((3, 4 * B, B), BF),
            pltpu.VMEM((2, 2 * B, B), BF),
            pltpu.SemaphoreType.DMA((3 * CH + 1,)),
            pltpu.SemaphoreType.DMA,
            pltpu.SemaphoreType.DMA((len(LINK_OPS),)),
            pltpu.SemaphoreType.DMA,
            pltpu.SemaphoreType.DMA((len(CORE_OPS),)),
            pltpu.SemaphoreType.DMA,
            pltpu.SemaphoreType.DMA((len(Z_STEPS),)),
            pltpu.SemaphoreType.DMA((len(SUMS),)),
        ],
        compiler_params=pltpu.CompilerParams(
            collective_id=0, has_side_effects=True, vmem_limit_bytes=58_000_000
        ),
        name="gather_update_exchange",
    )(lrank, urank, halves, shifts, xin, yin, pin, qin)


def per_device(lower_basis, lower_coeff, upper_basis, upper_coeff, lower_rank, upper_rank, child_half, owner_shift):
    blocks = main_call(
        lower_basis[0, 0], lower_coeff[0, 0], upper_basis[0, 0], upper_coeff[0, 0],
        lower_rank[0, 0], upper_rank[0, 0], child_half, owner_shift,
    )
    return blocks.reshape(1, 1, 16 * B, B)


def solution(mesh):
    whole = P("front", "tile", None, None)
    ranks = P("front", "tile", None)
    return jax.shard_map(
        per_device,
        mesh=mesh,
        in_specs=(whole, whole, whole, whole, ranks, ranks, P(), P()),
        out_specs=whole,
        check_vma=False,
    )
```
